128 devices in a mesh: tok: 16 (over z, x), mp: 8 (over y, core).
Axes of the slice: x: 4, y: 4, z: 4, core: 2. Of those that a mesh axis runs over, the one named last changes fastest.
Arguments:
- tokens: bfloat16 [6144, 2048], P('tok', 'mp'), may hold values from -120 to 120
- norm_gain: float32 [2048], replicated, may hold values from 0.5 to 1.5
- running_sq: float32 [2048], P('mp'), may hold values from 0.5 to 4
- gate_weight: bfloat16 [2048, 8192], P(None, 'mp'), may hold values from -0.125 to 0.125
- up_weight: bfloat16 [2048, 8192], P(None, 'mp'), may hold values from -0.125 to 0.125
- down_weight_t: bfloat16 [2048, 8192], P(None, 'mp'), may hold values from -0.0625 to 0.0625
- groups: int32 [384], P('tok'), may hold values from 0 to 47, as said below
- cotangent: bfloat16 [6144, 2048], P('tok', 'mp'), may hold values from -6 to 6
Outputs:
- block_out: bfloat16 [6144, 2048], P('tok', 'mp')
- grad_tokens: bfloat16 [6144, 2048], P('tok', 'mp')
- running_new: float32 [2048], P('mp')
- grad_gain: float32 [2048], P('mp')
- grad_gate: float32 [2048, 8192], P('tok', 'mp')
- grad_up: float32 [2048, 8192], P('tok', 'mp')
- grad_down_t: float32 [2048, 8192], P('tok', 'mp')
The draws below stay inside these ranges and needn't reach their ends.
Inputs may be any that keep to these rules, and one draw needn't show every extreme that they name: Each of the 48 ghost groups holds exactly 8 blocks.
All inputs are finite; a program needn't handle non-finite values.
Results may differ from the reference program's by a relative error of at most 0.02.
Values may be sent and summed in bfloat16 or wider, within the bound.
No kernel may reach another device: no remote copies, remote signals or barrier semaphores. Data moves between devices by JAX's collectives and lax.ppermute only.
A program may use at most 128 MiB of HBM per device.

```python
import math
import jax
import jax.numpy as jnp
from jax import lax

D = 2048
FF = 8192
GHOST = 128
BLK = 16
TOKENS = 6144
GROUPS = 48
NBLK = 384


def draw_groups(key, part):
    blocks_per_group = GHOST // BLK
    order = jax.random.permutation(jax.random.fold_in(key, 11), NBLK)
    return (order // blocks_per_group).astype(jnp.int32)


def draw_tokens(key, part):
    key_base, key_block, key_column = jax.random.split(jax.random.fold_in(key, 23), 3)
    position = jnp.arange(TOKENS, dtype=jnp.float32)
    rising = jnp.exp(jnp.log(3.0) * position / TOKENS)
    block_scale = jnp.exp(jax.random.uniform(key_block, (NBLK,), jnp.float32, jnp.log(0.5), jnp.log(2.0)))
    row_scale = jnp.broadcast_to(block_scale[:, None], (NBLK, BLK)).reshape(TOKENS) * rising
    column_scale = jnp.exp(jax.random.uniform(key_column, (D,), jnp.float32, jnp.log(0.3), jnp.log(3.0)))
    base = jnp.clip(jax.random.normal(key_base, (TOKENS, D), jnp.float32), -6.0, 6.0)
    return (base * row_scale[:, None] * column_scale[None, :]).astype(jnp.bfloat16)


def level_of(stream_key, dims, pieces, low, top_value):
    def one(dim, shards_of):
        draws = jax.random.uniform(jax.random.fold_in(jax.random.fold_in(stream_key, 6), dim), (shards_of,), jnp.float32, low / len(pieces), top_value / len(pieces))
        return jnp.repeat(jnp.exp(draws), dims[dim] // shards_of).reshape((-1,) + (1,) * (len(dims) - dim - 1))

    loudness = one(*pieces[0])
    for cut in pieces[1:]:
        loudness = loudness * one(*cut)
    return loudness


def noise(rng, extent, width, bound, shards=(), kind=jnp.bfloat16):
    array = jax.random.normal(rng, extent, jnp.float32) * width
    if len(shards) > 0:
        array = level_of(rng, extent, shards, -0.22, 0.18) * array
    return jnp.clip(array, min=-bound, max=bound).astype(kind)


def setup_inputs(seed: int = 0) -> dict:
    key_of = jax.random.split(jax.random.key(seed), 9)
    return {
        "tokens": draw_tokens(jax.random.fold_in(key_of[8], 71), 0),
        "norm_gain": jnp.clip(1.0 + 0.1 * jax.random.normal(key_of[1], (D,), jnp.float32), 0.5, 1.5),
        "running_sq": jnp.clip(jnp.exp(math.log(4.0) - 2.0794415 * jax.random.uniform(key_of[2], (D,), jnp.float32) ** level_of(key_of[2], (D,), ((0, 8),), -0.2, 0.2)), 0.5, 4.0),
        "gate_weight": noise(key_of[3], (D, FF), D ** -0.5, 0.125, ((1, 8),)),
        "up_weight": noise(key_of[4], (D, FF), D ** -0.5, 0.125, ((1, 8),)),
        "down_weight_t": noise(key_of[5], (D, FF), FF ** -0.5, 0.0625, ((1, 8),)),
        "groups": draw_groups(jax.random.fold_in(key_of[8], 71), 0),
        "cotangent": noise(key_of[7], (TOKENS, D), 1.0, 6.0, ((0, 16), (1, 8))),
    }


epsilon = 1e-05
momentum = 0.1
highest = lax.Precision.HIGHEST

def group_onehot(groups):
    return (groups[None, :] == jnp.arange(GROUPS, dtype=jnp.int32)[:, None]).astype(jnp.float32)

def group_sums(values, onehot):
    blocks = values.reshape(values.shape[0] // BLK, BLK, values.shape[1]).sum(axis=1)
    return jnp.dot(onehot, blocks, precision=highest, preferred_element_type=jnp.float32)

def per_token(table, onehot):
    per_block = jnp.dot(onehot.T, table, precision=highest, preferred_element_type=jnp.float32)
    wide = jnp.broadcast_to(per_block[:, None, :], (per_block.shape[0], BLK, per_block.shape[1]))
    return wide.reshape(per_block.shape[0] * BLK, per_block.shape[1])

def reference(tokens, norm_gain, running_sq, gate_weight, up_weight, down_weight_t, groups, cotangent):
    onehot = group_onehot(groups)
    x_float = tokens.astype(jnp.float32)
    quad_mean = group_sums(x_float * x_float, onehot) / GHOST
    scale = per_token(lax.rsqrt(quad_mean + epsilon), onehot)
    normed = x_float * scale
    hid_in = (norm_gain * normed).astype(jnp.bfloat16)
    gate = jnp.dot(hid_in, gate_weight, preferred_element_type=jnp.float32)
    lift = jnp.dot(hid_in, up_weight, preferred_element_type=jnp.float32)
    sigma = jax.nn.sigmoid(gate)
    hidden = (gate * sigma * lift).astype(jnp.bfloat16)
    branch = lax.dot_general(hidden, down_weight_t, (((1,), (1,)), ((), ())), preferred_element_type=jnp.float32)
    block_out = (x_float + branch).astype(jnp.bfloat16)
    running_new = (1.0 - momentum) * running_sq + momentum * lax.optimization_barrier(jnp.mean(quad_mean, axis=0))
    grad_down_t = lax.dot_general(cotangent, hidden, (((0,), (0,)), ((), ())), preferred_element_type=jnp.float32)
    grad_hidden = jnp.dot(cotangent, down_weight_t, preferred_element_type=jnp.float32)
    grad_gate_in = (grad_hidden * lift * sigma * (1.0 + gate * (1.0 - sigma))).astype(jnp.bfloat16)
    grad_lift = (grad_hidden * gate * sigma).astype(jnp.bfloat16)
    grad_gate = lax.dot_general(hid_in, grad_gate_in, (((0,), (0,)), ((), ())), preferred_element_type=jnp.float32)
    grad_up = lax.dot_general(hid_in, grad_lift, (((0,), (0,)), ((), ())), preferred_element_type=jnp.float32)
    grad_normed_in = lax.dot_general(grad_gate_in, gate_weight, (((1,), (1,)), ((), ())), preferred_element_type=jnp.float32)
    grad_normed_in = grad_normed_in + lax.dot_general(grad_lift, up_weight, (((1,), (1,)), ((), ())), preferred_element_type=jnp.float32)
    partial_value = group_sums(grad_normed_in * normed, onehot)
    grad_gain = lax.optimization_barrier(jnp.sum(partial_value, axis=0))
    mean_term = per_token(norm_gain * partial_value / GHOST, onehot)
    grad_tokens = (cotangent.astype(jnp.float32) + scale * (norm_gain * grad_normed_in - normed * mean_term)).astype(jnp.bfloat16)
    return (block_out, grad_tokens, running_new, grad_gain, grad_gate, grad_up, grad_down_t)
```

```python
import jax
import jax.numpy as jnp
from jax import lax
from jax.experimental import pallas as pl
from jax.experimental.pallas import tpu as pltpu
from jax.sharding import Mesh
from jax.sharding import PartitionSpec as P

GHOST = 128
BLK = 16
RING = 4
NEAR = [(i, i ^ 1) for i in range(RING)]
FAR = [(i, RING - 1 - i) for i in range(RING)]
CORES = [(0, 1), (1, 0)]
EPSILON = 1e-05
MOMENTUM = 0.1
HIGHEST = lax.Precision.HIGHEST


bf16 = jnp.bfloat16
f32 = jnp.float32


def shift(k):
    return [(i, (i + k) % RING) for i in range(RING)]


def ring_sum(x, axis):
    others = [lax.ppermute(x, axis, shift(k)) for k in (1, 3, 2)]
    return (x + others[0]) + (others[1] + others[2])


def tok_sum(x):
    return ring_sum(ring_sum(x, "z"), "x")


def group_sums(values, onehot):
    blocks = values.reshape(values.shape[0] // BLK, BLK, values.shape[1]).sum(axis=1)
    return jnp.dot(onehot, blocks, precision=HIGHEST, preferred_element_type=f32)


def per_token(table, onehot):
    per_block = jnp.dot(onehot.T, table, precision=HIGHEST, preferred_element_type=f32)
    wide = jnp.broadcast_to(per_block[:, None, :], (per_block.shape[0], BLK, per_block.shape[1]))
    return wide.reshape(per_block.shape[0] * BLK, per_block.shape[1])


def vmem_spec():
    return pl.BlockSpec(memory_space=pltpu.VMEM)


def smem_spec():
    return pl.BlockSpec(memory_space=pltpu.SMEM)


def gathered(x):
    near = [x] + [lax.ppermute(x, "y", shift(-k)) for k in (1, 2, 3)]
    far = [lax.ppermute(v, "c", CORES) for v in near]
    return near + far


def assemble_kernel(place, *refs):
    pieces, out = refs[:-1], refs[-1]
    width = pieces[0].shape[1]
    for i, piece in enumerate(pieces):
        out[:, pl.ds(pl.multiple_of(place[i] * width, width), width)] = piece[...]


def assembled(pieces, place):
    rows, width = pieces[0].shape
    return pl.pallas_call(
        assemble_kernel,
        out_shape=jax.ShapeDtypeStruct((rows, width * len(pieces)), pieces[0].dtype),
        in_specs=[smem_spec()] + [vmem_spec()] * len(pieces),
        out_specs=vmem_spec(),
        name="assemble",
    )(place, *pieces)


def contract_rows(left, right):
    return lax.dot_general(left, right, (((0,), (0,)), ((), ())), preferred_element_type=f32)


def contract_cols(left, right):
    return lax.dot_general(left, right, (((1,), (1,)), ((), ())), preferred_element_type=f32)


def rows_product(order, left, right, send, keep):
    half = send.shape[0] // 128
    for i in range(2 * half):
        block = left[:, pl.ds(pl.multiple_of(order[i] * 128, 128), 128)]
        value = contract_rows(block, right).astype(send.dtype)
        if i < half:
            send[i * 128 : (i + 1) * 128, :] = value
        else:
            keep[(i - half) * 128 : (i - half + 1) * 128, :] = value


def hidden_kernel(order, hid, dy, gate_w, up_w, down_w, hidden, ggi, gl, send, keep):
    gate = jnp.dot(hid[...], gate_w[...], preferred_element_type=f32)
    lift = jnp.dot(hid[...], up_w[...], preferred_element_type=f32)
    grad = jnp.dot(dy[...], down_w[...], preferred_element_type=f32)
    sigma = jax.nn.sigmoid(gate)
    act = gate * sigma
    hidden[...] = (act * lift).astype(bf16)
    ggi[...] = (grad * lift * sigma * (1.0 + gate * (1.0 - sigma))).astype(bf16)
    gl[...] = (grad * act).astype(bf16)
    rows_product(order, dy, hidden[...], send, keep)


def hidden_part(p, order, hid, dy, gate_w, up_w, down_w):
    rows, width = hid.shape
    part = gate_w.shape[1] // RING
    whole = pl.BlockSpec((rows, width), lambda i: (0, 0))
    weight = pl.BlockSpec((width, part), lambda i: (0, p))
    act = jax.ShapeDtypeStruct((rows, part), bf16)
    half = jax.ShapeDtypeStruct((width // 2, part), bf16)
    return pl.pallas_call(
        hidden_kernel,
        grid=(1,),
        out_shape=(act, act, act, half, half),
        in_specs=[smem_spec(), whole, whole, weight, weight, weight],
        out_specs=(
            pl.BlockSpec((rows, part), lambda i: (0, 0)),
            pl.BlockSpec((rows, part), lambda i: (0, 0)),
            pl.BlockSpec((rows, part), lambda i: (0, 0)),
            pl.BlockSpec((width // 2, part), lambda i: (0, 0)),
            pl.BlockSpec((width // 2, part), lambda i: (0, 0)),
        ),
        name="hidden_part",
    )(order, hid, dy, gate_w, up_w, down_w)


def grads_kernel(order, hid, ggi, gl, send, keep):
    both = jnp.concatenate([ggi[...], gl[...]], axis=1)
    rows_product(order, hid, both, send, keep)


def grads_part(order, hid, ggi, gl):
    width = hid.shape[1]
    half = jax.ShapeDtypeStruct((width // 2, 2 * ggi.shape[1]), bf16)
    return pl.pallas_call(
        grads_kernel,
        out_shape=(half, half),
        in_specs=[smem_spec(), vmem_spec(), vmem_spec(), vmem_spec()],
        out_specs=(vmem_spec(), vmem_spec()),
        name="grads_part",
    )(order, hid, ggi, gl)


def back_kernel(pairs):
    def kernel(place, *refs):
        acts = refs[: pairs * RING]
        weights = refs[pairs * RING : pairs * RING + pairs]
        far, near = refs[pairs * RING + pairs :]
        total = None
        for j in range(pairs):
            act = jnp.concatenate([r[...] for r in acts[j * RING : (j + 1) * RING]], axis=1)
            term = contract_cols(act, weights[j][...])
            total = term if total is None else total + term
        value = total.astype(bf16)[None]
        i = pl.program_id(0)

        @pl.when(i < RING)
        def _():
            far[...] = value

        @pl.when(i >= RING)
        def _():
            near[...] = value

    return kernel


def back(place, acts, weights):
    rows, part = acts[0][0].shape
    hidden_width = weights[0].shape[1]
    feat = weights[0].shape[0] // (2 * RING)
    pairs = len(weights)
    out = jax.ShapeDtypeStruct((RING, rows, feat), bf16)
    return pl.pallas_call(
        back_kernel(pairs),
        grid_spec=pltpu.PrefetchScalarGridSpec(
            num_scalar_prefetch=1,
            grid=(2 * RING,),
            in_specs=[pl.BlockSpec((rows, part), lambda i, s: (0, 0))] * (pairs * RING)
            + [pl.BlockSpec((feat, hidden_width), lambda i, s: (s[i], 0))] * pairs,
            out_specs=(
                pl.BlockSpec((1, rows, feat), lambda i, s: (jnp.minimum(i, RING - 1), 0, 0)),
                pl.BlockSpec((1, rows, feat), lambda i, s: (jnp.maximum(i - RING, 0), 0, 0)),
            ),
        ),
        out_shape=(out, out),
        name="back",
    )(place, *[a for group in acts for a in group], *weights)


def mp_scattered(far, near):
    other = lax.ppermute(far, "c", CORES)
    both = [(near[k].astype(f32) + other[k].astype(f32)) for k in range(RING)]
    came = [lax.ppermute(both[k].astype(bf16), "y", shift(k)).astype(f32) for k in range(1, RING)]
    return (both[0] + came[0]) + (came[1] + came[2])


def added(keep, came):
    return (keep.astype(f32) + came.astype(f32)).astype(bf16)


def split_add(keep, came):
    half = keep.shape[0] // 2
    return added(keep[:half], came[:half]), added(keep[half:], came[half:])


def body(tokens, norm_gain, running_sq, gate_weight, up_weight, down_weight_t, groups, cotangent):
    tok_rows, feat = tokens.shape
    groups_total = tok_rows * RING * RING // GHOST
    z, x, y, c = (lax.axis_index(a) for a in ("z", "x", "y", "c"))
    onehot = (groups[None, :] == jnp.arange(groups_total, dtype=jnp.int32)[:, None]).astype(f32)
    steps = jnp.arange(RING, dtype=jnp.int32)
    ring_y = (y + steps) % RING
    place = jnp.concatenate([2 * ring_y + c, 2 * ring_y + (1 - c)])
    place_back = jnp.concatenate([2 * ring_y + (1 - c), 2 * ring_y + c])

    def halving(i, first):
        p = i ^ 1 if first == 0 else RING - 1 - i
        q = RING - 1 - i if first == 0 else i ^ 1
        far_q = RING - 1 - p if first == 0 else p ^ 1
        return jnp.stack([far_q, p, q, i])

    orders = []
    for major, first in (("z", 0), ("z", 1), ("x", 0), ("x", 1)):
        hz, hx = halving(z, first), halving(x, first)
        if major == "z":
            orders.append((RING * hz[:, None] + hx[None, :]).reshape(-1))
        else:
            orders.append((RING * hz[None, :] + hx[:, None]).reshape(-1))

    x_local = tokens.astype(f32)
    gain_local = lax.dynamic_slice_in_dim(norm_gain, (2 * y + c) * feat, feat, 0)
    quad_mean = tok_sum(group_sums(x_local * x_local, onehot)) / GHOST
    dy_full = assembled(gathered(cotangent), place)
    scale = per_token(lax.rsqrt(quad_mean + EPSILON), onehot)
    normed = x_local * scale
    hid_full = assembled(gathered((gain_local * normed).astype(bf16)), place)
    running_new = (1.0 - MOMENTUM) * running_sq + MOMENTUM * jnp.mean(quad_mean, axis=0)

    parts = [
        hidden_part(p, orders[p], hid_full, dy_full, gate_weight, up_weight, down_weight_t)
        for p in range(RING)
    ]
    routes = []
    for major, first in (("z", 0), ("z", 1), ("x", 0), ("x", 1)):
        minor = "x" if major == "z" else "z"
        pair = (NEAR, FAR) if first == 0 else (FAR, NEAR)
        routes.append(((major, pair[0]), (major, pair[1]), (minor, pair[0]), (minor, pair[1])))

    sums = []
    for p in range(RING):
        hidden, ggi, gl, send_d, keep_d = parts[p]
        send_g, keep_g = grads_part(orders[p], hid_full, ggi, gl)
        r1, r2, r3, r4 = routes[p]
        came_d = lax.ppermute(send_d, *r1)
        came_g = lax.ppermute(send_g, *r1)
        send_d, keep_d = split_add(keep_d, came_d)
        came_d = lax.ppermute(send_d, *r2)
        send_g, keep_g = split_add(keep_g, came_g)
        came_g = lax.ppermute(send_g, *r2)
        keep = jnp.concatenate([keep_d, keep_g], axis=1)
        came = jnp.concatenate([came_d, came_g], axis=1)
        send, keep = split_add(keep, came)
        came = lax.ppermute(send, *r3)
        send, keep = split_add(keep, came)
        came = lax.ppermute(send, *r4)
        sums.append(keep.astype(f32) + came.astype(f32))
    part = gate_weight.shape[1] // RING
    grad_down_t = jnp.concatenate([s[:, :part] for s in sums], axis=1)
    grad_gate = jnp.concatenate([s[:, part : 2 * part] for s in sums], axis=1)
    grad_up = jnp.concatenate([s[:, 2 * part :] for s in sums], axis=1)

    far, near = back(place_back, [[q[1] for q in parts], [q[2] for q in parts]], [gate_weight, up_weight])
    grad_normed_in = mp_scattered(far, near)
    partial_value = tok_sum(group_sums(grad_normed_in * normed, onehot))
    grad_gain = jnp.sum(partial_value, axis=0)
    mean_term = per_token(gain_local * partial_value / GHOST, onehot)
    grad_tokens = (
        cotangent.astype(f32) + scale * (gain_local * grad_normed_in - normed * mean_term)
    ).astype(bf16)

    far, near = back(place_back, [[q[0] for q in parts]], [down_weight_t])
    block_out = (x_local + mp_scattered(far, near)).astype(bf16)
    return (block_out, grad_tokens, running_new, grad_gain, grad_gate, grad_up, grad_down_t)


def solution(mesh):
    torus = Mesh(mesh.devices.reshape(RING, RING, RING, 2), ("z", "x", "y", "c"))
    tok, mp = ("z", "x"), ("y", "c")
    placed = (P(tok, mp), P(), P(mp), P(None, mp), P(None, mp), P(None, mp), P(tok), P(tok, mp))
    out = (P(tok, mp), P(tok, mp), P(mp), P(mp), P(tok, mp), P(tok, mp), P(tok, mp))
    return jax.shard_map(body, mesh=torus, in_specs=placed, out_specs=out, check_vma=False)
```

```python
import jax
import jax.numpy as jnp
from jax import lax
from jax.experimental import pallas as pl
from jax.experimental.pallas import tpu as pltpu
from jax.sharding import Mesh
from jax.sharding import PartitionSpec as P


GHOST = 128
BLK = 16
RING = 4
NEAR = [(i, i ^ 1) for i in range(RING)]
FAR = [(i, RING - 1 - i) for i in range(RING)]
CORES = [(0, 1), (1, 0)]
EPSILON = 1e-05
MOMENTUM = 0.1


bf16 = jnp.bfloat16
f32 = jnp.float32


PATTERNS = (("z", 0), ("z", 1), ("x", 0), ("x", 1))


def halving(i, first):
    near, far = i ^ 1, RING - 1 - i
    p, q = (near, far) if first == 0 else (far, near)
    return [RING - 1 - p if first == 0 else p ^ 1, p, q, i]


def row_blocks(coords, pattern):
    major, first = pattern
    hz, hx = halving(coords[0], first), halving(coords[1], first)
    if major == "z":
        return [RING * a + b for a in hz for b in hx]
    return [RING * a + b for b in hx for a in hz]


def feature_blocks(coords, other):
    core = coords[3] if other == 0 else 1 - coords[3]
    return [2 * ((coords[2] + k) & (RING - 1)) + core for k in range(RING)]


def shift(k):
    return [(i, (i + k) % RING) for i in range(RING)]


def to_all(x):
    return lax.all_to_all(x, ("z", "x"), 0, 0, tiled=True)


def vmem_spec():
    return pl.BlockSpec(memory_space=pltpu.VMEM)


def smem_spec():
    return pl.BlockSpec(memory_space=pltpu.SMEM)


def gathered(x):
    near = [x]
    for k in (1, 3, 2):
        near.append(lax.ppermute(x, "y", shift(-k)))
    near = [near[0], near[1], near[3], near[2]]
    far = []
    for k in range(RING):
        far.append(lax.ppermute(near[k], "c", CORES))
    return near + far


def block_sum(value):
    return jnp.sum(value, axis=0, keepdims=True)


def spread(acc, out):
    table = acc[...].astype(bf16)
    for i in range(out.shape[0]):
        out[i] = table


def own_gain(coords, gain, feat):
    return gain[:, pl.ds(pl.multiple_of((2 * coords[2] + coords[3]) * feat, feat), feat)]


def received_sum(received):
    total = received[0].astype(f32)
    for i in range(1, received.shape[0]):
        total = total + received[i].astype(f32)
    return total


def stats_kernel(groups, tokens, out, acc):
    acc[...] = jnp.zeros_like(acc)
    for b in range(tokens.shape[0] // BLK):
        value = tokens[b * BLK : (b + 1) * BLK, :].astype(f32)
        row = pl.ds(groups[b], 1)
        acc[row, :] = acc[row, :] + block_sum(value * value)
    spread(acc, out)


def stats(groups, tokens, groups_total):
    feat = tokens.shape[1]
    return pl.pallas_call(
        stats_kernel,
        out_shape=jax.ShapeDtypeStruct((RING * RING, groups_total, feat), bf16),
        in_specs=[smem_spec(), vmem_spec()],
        out_specs=vmem_spec(),
        scratch_shapes=[pltpu.VMEM((groups_total, feat), f32)],
        compiler_params=limits(4),
        name="stats",
    )(groups, tokens)


def norm_kernel(groups, coords, tokens, gain, running, received, hid, table, running_new):
    quad_mean = received_sum(received) * (1.0 / GHOST)
    table[...] = lax.rsqrt(quad_mean + EPSILON)
    mean = jnp.sum(quad_mean, axis=0, keepdims=True) / quad_mean.shape[0]
    running_new[...] = (1.0 - MOMENTUM) * running[...] + MOMENTUM * mean
    gain_row = own_gain(coords, gain, tokens.shape[1])
    for b in range(tokens.shape[0] // BLK):
        rows = slice(b * BLK, (b + 1) * BLK)
        scale = table[pl.ds(groups[b], 1), :]
        hid[rows, :] = (gain_row * (tokens[rows, :].astype(f32) * scale)).astype(bf16)


def normalized(groups, coords, tokens, gain, running, received):
    groups_total = received.shape[1]
    rows, feat = tokens.shape
    return pl.pallas_call(
        norm_kernel,
        out_shape=(
            jax.ShapeDtypeStruct((rows, feat), bf16),
            jax.ShapeDtypeStruct((groups_total, feat), f32),
            jax.ShapeDtypeStruct((1, feat), f32),
        ),
        in_specs=[smem_spec(), smem_spec()] + [vmem_spec()] * 4,
        out_specs=(vmem_spec(),) * 3,
        compiler_params=limits(4),
        name="normalized",
    )(groups, coords, tokens, gain, running, received)


def partial_kernel(groups, tokens, table, own, *refs):
    came, (grad, out, acc) = refs[:-3], refs[-3:]
    total = own[...]
    for ref in came:
        total = total + ref[...].astype(f32)
    grad[...] = total.T
    acc[...] = jnp.zeros_like(acc)
    for b in range(tokens.shape[0] // BLK):
        rows = slice(b * BLK, (b + 1) * BLK)
        row = pl.ds(groups[b], 1)
        normed = tokens[rows, :].astype(f32) * table[row, :]
        acc[row, :] = acc[row, :] + block_sum(grad[rows, :] * normed)
    spread(acc, out)


def partials(groups, tokens, table, own, came):
    rows, feat = tokens.shape
    return pl.pallas_call(
        partial_kernel,
        out_shape=(
            jax.ShapeDtypeStruct((rows, feat), f32),
            jax.ShapeDtypeStruct((RING * RING, *table.shape), bf16),
        ),
        in_specs=[smem_spec()] + [vmem_spec()] * (3 + len(came)),
        out_specs=(vmem_spec(),) * 2,
        scratch_shapes=[pltpu.VMEM(table.shape, f32)],
        compiler_params=limits(6),
        name="partials",
    )(groups, tokens, table, own, *came)


def input_kernel(groups, coords, tokens, cotangent, gain, table, grad, received, out, grad_gain, acc):
    partial = received_sum(received)
    grad_gain[...] = jnp.sum(partial, axis=0, keepdims=True)
    gain_row = own_gain(coords, gain, tokens.shape[1])
    acc[...] = gain_row * partial * (1.0 / GHOST)
    for b in range(tokens.shape[0] // BLK):
        rows = slice(b * BLK, (b + 1) * BLK)
        row = pl.ds(groups[b], 1)
        scale = table[row, :]
        normed = tokens[rows, :].astype(f32) * scale
        inner = gain_row * grad[rows, :] - normed * acc[row, :]
        out[rows, :] = (cotangent[rows, :].astype(f32) + scale * inner).astype(bf16)


def input_grads(groups, coords, tokens, cotangent, gain, table, grad, received):
    rows, feat = tokens.shape
    return pl.pallas_call(
        input_kernel,
        out_shape=(
            jax.ShapeDtypeStruct((rows, feat), bf16),
            jax.ShapeDtypeStruct((1, feat), f32),
        ),
        in_specs=[smem_spec(), smem_spec()] + [vmem_spec()] * 6,
        out_specs=(vmem_spec(),) * 2,
        scratch_shapes=[pltpu.VMEM(table.shape, f32)],
        compiler_params=limits(6),
        name="input_grads",
    )(groups, coords, tokens, cotangent, gain, table, grad, received)


def branch_kernel(tokens, own, *refs):
    came, out = refs[:-1], refs[-1]
    total = own[...]
    for ref in came:
        total = total + ref[...].astype(f32)
    out[...] = (tokens[...].astype(f32) + total.T).astype(bf16)


def branch_out(tokens, own, came):
    return pl.pallas_call(
        branch_kernel,
        out_shape=jax.ShapeDtypeStruct(tokens.shape, bf16),
        in_specs=[vmem_spec()] * (2 + len(came)),
        out_specs=vmem_spec(),
        compiler_params=limits(6),
        name="branch_out",
    )(tokens, own, *came)


def grad_kernel(dy, weight, out):
    out[...] = jnp.dot(dy[...], weight[...], preferred_element_type=f32)


def hidden_grads(dy, weight):
    rows, width = dy.shape
    hidden = weight.shape[1]
    part = hidden // RING
    return pl.pallas_call(
        grad_kernel,
        grid=(RING,),
        out_shape=jax.ShapeDtypeStruct((rows, hidden), f32),
        in_specs=[
            pl.BlockSpec((rows, width), lambda i: (0, 0)),
            pl.BlockSpec((width, part), lambda i: (0, i)),
        ],
        out_specs=pl.BlockSpec((rows, part), lambda i: (0, i)),
        compiler_params=limits(12),
        name="hidden_grads",
    )(dy, weight)


def limits(mib):
    return pltpu.CompilerParams(vmem_limit_bytes=mib << 20)


def assemble_kernel(coords, *refs):
    pieces, (out, turned) = refs[:-2], refs[-2:]
    width = pieces[0].shape[1]
    places = feature_blocks(coords, 0) + feature_blocks(coords, 1)
    for place, piece in zip(places, pieces):
        first = pl.multiple_of(place * width, width)
        out[:, pl.ds(first, width)] = piece[...]
        turned[pl.ds(first, width), :] = piece[...].T


def assembled(coords, pieces):
    rows, width = pieces[0].shape
    total = width * len(pieces)
    return pl.pallas_call(
        assemble_kernel,
        out_shape=(
            jax.ShapeDtypeStruct((rows, total), bf16),
            jax.ShapeDtypeStruct((total, rows), bf16),
        ),
        in_specs=[smem_spec()] + [vmem_spec()] * len(pieces),
        out_specs=(vmem_spec(), vmem_spec()),
        compiler_params=limits(10),
        name="assemble",
    )(coords, *pieces)


def rows_product(blocks, turned, right, send, keep, first):
    columns = slice(first, first + right.shape[1])
    half = len(blocks) // 2
    for part, out in ((blocks[:half], send), (blocks[half:], keep)):
        left = jnp.concatenate(
            [turned[pl.ds(pl.multiple_of(b * 128, 128), 128), :] for b in part], axis=0
        )
        out[:, columns] = jnp.dot(left, right, preferred_element_type=f32).astype(out.dtype)


def hidden_kernel(pattern):
    def kernel(coords, hid, hid_t, dy_t, grad_in, gate_w, up_w, hidden_t, ggi_t, gl_t, send, keep):
        gate = jnp.dot(hid[...], gate_w[...], preferred_element_type=f32)
        lift = jnp.dot(hid[...], up_w[...], preferred_element_type=f32)
        grad = grad_in[...]
        sigma = jax.nn.sigmoid(gate)
        act = gate * sigma
        hidden = (act * lift).astype(bf16)
        ggi = (grad * lift * sigma * (1.0 + gate * (1.0 - sigma))).astype(bf16)
        gl = (grad * act).astype(bf16)
        part = gate.shape[1]
        blocks = row_blocks(coords, pattern)
        rows_product(blocks, dy_t, hidden, send, keep, 0)
        rows_product(blocks, hid_t, jnp.concatenate([ggi, gl], axis=1), send, keep, part)
        hidden_t[...] = hidden.T
        ggi_t[...] = ggi.T
        gl_t[...] = gl.T

    return kernel


def hidden_part(p, coords, hid, hid_t, dy_t, grad_in, gate_w, up_w):
    rows, width = hid.shape
    part = gate_w.shape[1] // RING

    def fixed(*shape):
        return pl.BlockSpec(shape, lambda i: (0, 0))

    weight = pl.BlockSpec((width, part), lambda i: (0, p))
    act = jax.ShapeDtypeStruct((part, rows), bf16)
    half = jax.ShapeDtypeStruct((width // 2, 3 * part), bf16)
    return pl.pallas_call(
        hidden_kernel(PATTERNS[p]),
        grid=(1,),
        out_shape=(act, act, act, half, half),
        in_specs=[
            smem_spec(),
            fixed(rows, width),
            fixed(width, rows),
            fixed(width, rows),
            pl.BlockSpec((rows, part), lambda i: (0, p)),
            weight,
            weight,
        ],
        out_specs=(fixed(part, rows),) * 3 + (fixed(width // 2, 3 * part),) * 2,
        compiler_params=limits(20),
        name="hidden_part",
    )(coords, hid, hid_t, dy_t, grad_in, gate_w, up_w)


def back_kernel(pairs):
    def kernel(coords, *refs):
        acts = refs[: pairs * RING]
        weights = refs[pairs * RING : pairs * RING + pairs]
        outs = refs[pairs * RING + pairs :]
        feat = outs[0].shape[1]
        for other, out in ((1, outs[0]), (0, outs[1])):
            total = None
            for j in range(pairs):
                act = jnp.concatenate([r[...] for r in acts[j * RING : (j + 1) * RING]], axis=0)
                left = jnp.concatenate(
                    [
                        weights[j][pl.ds(pl.multiple_of(b * feat, feat), feat), :]
                        for b in feature_blocks(coords, other)
                    ],
                    axis=0,
                )
                term = jnp.dot(left, act, preferred_element_type=f32)
                total = term if total is None else total + term
            for k in range(RING):
                out[k] = total[k * feat : (k + 1) * feat, :].astype(bf16)

    return kernel


def back(coords, acts, weights):
    rows = acts[0][0].shape[1]
    feat = weights[0].shape[0] // (2 * RING)
    pairs = len(weights)
    out = jax.ShapeDtypeStruct((RING, feat, rows), bf16)
    return pl.pallas_call(
        back_kernel(pairs),
        in_specs=[smem_spec()] + [vmem_spec()] * (pairs * RING + pairs),
        out_specs=(vmem_spec(), vmem_spec()),
        out_shape=(out, out),
        compiler_params=limits(20),
        name="back",
    )(coords, *[a for group in acts for a in group], *weights)


def chip_sum_kernel(near, other, own, *sends):
    own[...] = near[0].astype(f32) + other[0].astype(f32)
    for k, send in enumerate(sends, 1):
        send[...] = (near[k].astype(f32) + other[k].astype(f32)).astype(bf16)


def mp_scattered(far, near):
    other = lax.ppermute(far, "c", CORES)
    piece = near.shape[1:]
    own, *sends = pl.pallas_call(
        chip_sum_kernel,
        out_shape=(jax.ShapeDtypeStruct(piece, f32),)
        + (jax.ShapeDtypeStruct(piece, bf16),) * (RING - 1),
        in_specs=[vmem_spec()] * 2,
        out_specs=(vmem_spec(),) * RING,
        compiler_params=limits(6),
        name="chip_sum",
    )(near, other)
    came = []
    for k in (1, 3, 2):
        came.append(lax.ppermute(sends[k - 1], "y", shift(k)))
    return own, came


def split_kernel(keep, came, send, kept):
    half = send.shape[0]
    send[...] = (keep[:half, :].astype(f32) + came[:half, :].astype(f32)).astype(bf16)
    kept[...] = (keep[half:, :].astype(f32) + came[half:, :].astype(f32)).astype(bf16)


def split_add(keep, came):
    half = jax.ShapeDtypeStruct((keep.shape[0] // 2, keep.shape[1]), bf16)
    return pl.pallas_call(
        split_kernel,
        out_shape=(half, half),
        in_specs=[vmem_spec()] * 2,
        out_specs=(vmem_spec(),) * 2,
        compiler_params=limits(8),
        name="split_add",
    )(keep, came)


def finish_kernel(*refs):
    ins, outs = refs[: 2 * RING], refs[2 * RING :]
    for p in range(RING):
        total = ins[2 * p][...].astype(f32) + ins[2 * p + 1][...].astype(f32)
        part = total.shape[1] // len(outs)
        for j, out in enumerate(outs):
            out[:, p * part : (p + 1) * part] = total[:, j * part : (j + 1) * part]


def finished(pairs):
    rows, width = pairs[0][0].shape
    out = jax.ShapeDtypeStruct((rows, width // 3 * RING), f32)
    return pl.pallas_call(
        finish_kernel,
        out_shape=(out,) * 3,
        in_specs=[vmem_spec()] * (2 * RING),
        out_specs=(vmem_spec(),) * 3,
        compiler_params=limits(6),
        name="finished",
    )(*[a for pair in pairs for a in pair])


def body(tokens, norm_gain, running_sq, gate_weight, up_weight, down_weight_t, groups, cotangent):
    tok_rows, feat = tokens.shape
    groups_total = tok_rows * RING * RING // GHOST
    coords = jnp.stack([lax.axis_index(a) for a in ("z", "x", "y", "c")]).astype(jnp.int32)
    gain = norm_gain.reshape(1, -1)
    local = stats(groups, tokens, groups_total)
    received = to_all(local)
    dy_pieces = gathered(cotangent)
    dy_full, dy_turned = assembled(coords, dy_pieces)
    hid, table, running_new = normalized(
        groups, coords, tokens, gain, running_sq.reshape(1, feat), received
    )
    hid_pieces = gathered(hid)
    grad_hidden = hidden_grads(dy_full, down_weight_t)
    hid_full, hid_turned = assembled(coords, hid_pieces)
    parts = []
    for p in range(RING):
        parts.append(
            hidden_part(
                p, coords, hid_full, hid_turned, dy_turned, grad_hidden, gate_weight, up_weight
            )
        )
    last = []
    for p, (major, first) in enumerate(PATTERNS):
        minor = "x" if major == "z" else "z"
        pair = (NEAR, FAR) if first == 0 else (FAR, NEAR)
        send, keep = parts[p][3:]
        for i, (axis, route) in enumerate(((major, 0), (major, 1), (minor, 0), (minor, 1)), 1):
            came = lax.ppermute(send, axis, pair[route])
            if i < 4:
                send, keep = split_add(keep, came)
        last.append((keep, came))
    grad_down_t, grad_gate, grad_up = finished(last)

    far, near = back(
        coords, [[q[1] for q in parts], [q[2] for q in parts]], [gate_weight, up_weight]
    )
    kept, came = mp_scattered(far, near)
    grad, local = partials(groups, tokens, table, kept, came)
    received = to_all(local)
    grad_tokens, grad_gain = input_grads(groups, coords, tokens, cotangent, gain, table, grad, received)

    far, near = back(coords, [[q[0] for q in parts]], [down_weight_t])
    kept, came = mp_scattered(far, near)
    block_out = branch_out(tokens, kept, came)
    return (
        block_out,
        grad_tokens,
        running_new.reshape(feat),
        grad_gain.reshape(feat),
        grad_gate,
        grad_up,
        grad_down_t,
    )


def solution(mesh):
    torus = Mesh(mesh.devices.reshape(RING, RING, RING, 2), ("z", "x", "y", "c"))
    tok, mp = ("z", "x"), ("y", "c")
    placed = (P(tok, mp), P(), P(mp), P(None, mp), P(None, mp), P(None, mp), P(tok), P(tok, mp))
    out = (P(tok, mp), P(tok, mp), P(mp), P(mp), P(tok, mp), P(tok, mp), P(tok, mp))

    return jax.shard_map(body, mesh=torus, in_specs=placed, out_specs=out, check_vma=False)
```

```python
import jax
import jax.numpy as jnp
from jax import lax
from jax.experimental import pallas as pl
from jax.experimental.pallas import tpu as pltpu
from jax.sharding import Mesh
from jax.sharding import PartitionSpec as P


GHOST = 128
BLK = 16
RING = 4
NEAR = [(i, i ^ 1) for i in range(RING)]
FAR = [(i, RING - 1 - i) for i in range(RING)]
CORES = [(0, 1), (1, 0)]
EPSILON = 1e-05
MOMENTUM = 0.1


bf16 = jnp.bfloat16
f32 = jnp.float32


PATTERNS = (("z", 0), ("z", 1), ("x", 0), ("x", 1))
LENT = 128


def halving(i, first):
    near, far = i ^ 1, RING - 1 - i
    p, q = (near, far) if first == 0 else (far, near)
    return [RING - 1 - p if first == 0 else p ^ 1, p, q, i]


def row_blocks(coords, pattern):
    major, first = pattern
    hz, hx = halving(coords[0], first), halving(coords[1], first)
    if major == "z":
        return [RING * a + b for a in hz for b in hx]
    return [RING * a + b for b in hx for a in hz]


def feature_blocks(coords, other):
    core = coords[3] if other == 0 else 1 - coords[3]
    return [2 * ((coords[2] + k) & (RING - 1)) + core for k in range(RING)]


def shift(k):
    return [(i, (i + k) % RING) for i in range(RING)]


def vmem_spec():
    return pl.BlockSpec(memory_space=pltpu.VMEM)


def smem_spec():
    return pl.BlockSpec(memory_space=pltpu.SMEM)


def in_hbm(x):
    return pltpu.with_memory_space_constraint(x, pltpu.HBM)


def gathered(x):
    near = [x]
    for k in (1, 3, 2):
        near.append(lax.ppermute(x, "y", shift(-k)))
    near = [near[0], near[1], near[3], near[2]]
    far = []
    for k in range(RING):
        far.append(lax.ppermute(near[k], "c", CORES))
    return near + far


def block_sum(value):
    return jnp.sum(value, axis=0, keepdims=True)


def own_gain(coords, gain, feat):
    return gain[:, pl.ds(pl.multiple_of((2 * coords[2] + coords[3]) * feat, feat), feat)]


def add_kernel(left, right, out):
    out[...] = left[...] + right[...]


def pair_added(left, right):
    return pl.pallas_call(
        add_kernel,
        out_shape=jax.ShapeDtypeStruct(left.shape, left.dtype),
        in_specs=[vmem_spec()] * 2,
        out_specs=vmem_spec(),
        compiler_params=limits(1),
        name="pair_added",
    )(left, right)


def tok_halves(x):
    for i, (axis, pairs) in enumerate((("z", NEAR), ("z", FAR), ("x", NEAR), ("x", FAR)), 1):
        came = lax.ppermute(x, axis, pairs)
        if i < 4:
            x = pair_added(x, came)
    return x, came


def ring_sum_kernel(*refs):
    ins, out = refs[:-1], refs[-1]
    out[...] = (ins[0][...] + ins[3][...]) + (ins[1][...] + ins[2][...])


def ring_pieces(x, axis):
    came = [x]
    for k in (1, 3, 2):
        came.append(lax.ppermute(x, axis, shift(k)))
    return came


def ring_sum(x, axis):
    pieces = ring_pieces(x, axis)
    return pl.pallas_call(
        ring_sum_kernel,
        out_shape=jax.ShapeDtypeStruct(x.shape, x.dtype),
        in_specs=[vmem_spec()] * RING,
        out_specs=vmem_spec(),
        compiler_params=limits(1),
        name="ring_sum",
    )(*pieces)


STAGE_CUTS = 4


def stage_kernel(*refs):
    count = (len(refs) - 1) // 2
    sems = refs[-1]
    copies = []
    for i in range(count):
        source, out = refs[i], refs[count + i]
        rows = source.shape[0] // STAGE_CUTS
        for j in range(STAGE_CUTS):
            part = pl.ds(j * rows, rows)
            copies.append(
                pltpu.make_async_copy(source.at[part], out.at[part], sems.at[i * STAGE_CUTS + j])
            )
    for copy in copies:
        copy.start()
    for copy in copies:
        copy.wait()


def staged(*weights):
    return pl.pallas_call(
        stage_kernel,
        out_shape=tuple(pltpu.VMEM(w.shape, w.dtype) for w in weights),
        in_specs=[pl.BlockSpec(memory_space=pltpu.HBM)] * len(weights),
        out_specs=(vmem_spec(),) * len(weights),
        scratch_shapes=[pltpu.SemaphoreType.DMA((STAGE_CUTS * len(weights),))],
        compiler_params=limits(1),
        name="staged",
    )(*[in_hbm(w) for w in weights])


def stats_kernel(groups, coords, tokens, cotangent, out, both):
    rows = tokens.shape[0]
    both[:rows, :] = tokens[...]
    both[rows:, :] = cotangent[...]
    out[...] = jnp.zeros_like(out)
    for b in range(rows // BLK):
        value = tokens[b * BLK : (b + 1) * BLK, :].astype(f32)
        row = pl.ds(groups[b], 1)
        out[row, :] = out[row, :] + block_sum(value * value)


def stats(groups, coords, tokens, cotangent, groups_total):
    rows, feat = tokens.shape
    return pl.pallas_call(
        stats_kernel,
        out_shape=(
            jax.ShapeDtypeStruct((groups_total, feat), f32),
            jax.ShapeDtypeStruct((2 * rows, feat), bf16),
        ),
        in_specs=[smem_spec(), smem_spec(), vmem_spec(), vmem_spec()],
        out_specs=(vmem_spec(),) * 2,
        compiler_params=limits(4),
        name="stats",
    )(in_hbm(groups), coords, in_hbm(tokens), in_hbm(cotangent))


def table_kernel(a, b, c, d, table, quad):
    quad_mean = ((a[...] + d[...]) + (b[...] + c[...])) * (1.0 / GHOST)
    quad[...] = quad_mean
    table[...] = lax.rsqrt(quad_mean + EPSILON)


def scale_table(pieces):
    out = jax.ShapeDtypeStruct(pieces[0].shape, f32)
    return pl.pallas_call(
        table_kernel,
        out_shape=(out, out),
        in_specs=[vmem_spec()] * RING,
        out_specs=(vmem_spec(),) * 2,
        compiler_params=limits(2),
        name="scale_table",
    )(*pieces)


def partial_kernel(groups, tokens, table, own, *refs):
    came, (grad, out) = refs[:-2], refs[-2:]
    total = own[...]
    for ref in came:
        total = total + ref[...].astype(f32)
    grad[...] = total.T
    out[...] = jnp.zeros_like(out)
    for b in range(tokens.shape[0] // BLK):
        rows = slice(b * BLK, (b + 1) * BLK)
        row = pl.ds(groups[b], 1)
        normed = tokens[rows, :].astype(f32) * table[row, :]
        out[row, :] = out[row, :] + block_sum(grad[rows, :] * normed)


def partials(groups, tokens, table, own, came):
    rows, feat = tokens.shape
    return pl.pallas_call(
        partial_kernel,
        out_shape=(
            jax.ShapeDtypeStruct((rows, feat), f32),
            jax.ShapeDtypeStruct(table.shape, f32),
        ),
        in_specs=[smem_spec()] + [vmem_spec()] * (3 + len(came)),
        out_specs=(vmem_spec(),) * 2,
        compiler_params=limits(6),
        name="partials",
    )(in_hbm(groups), tokens, table, own, *came)


def input_kernel(groups, coords, tokens, cotangent, gain, table, grad, mine, came, out, grad_gain, acc):
    partial = mine[...] + came[...]
    grad_gain[...] = jnp.sum(partial, axis=0, keepdims=True)
    gain_row = own_gain(coords, gain, tokens.shape[1])
    acc[...] = gain_row * partial * (1.0 / GHOST)
    for b in range(tokens.shape[0] // BLK):
        rows = slice(b * BLK, (b + 1) * BLK)
        row = pl.ds(groups[b], 1)
        scale = table[row, :]
        normed = tokens[rows, :].astype(f32) * scale
        inner = gain_row * grad[rows, :] - normed * acc[row, :]
        out[rows, :] = (cotangent[rows, :].astype(f32) + scale * inner).astype(bf16)


def input_grads(groups, coords, tokens, cotangent, gain, table, grad, mine, came):
    rows, feat = tokens.shape
    return pl.pallas_call(
        input_kernel,
        out_shape=(
            jax.ShapeDtypeStruct((rows, feat), bf16),
            jax.ShapeDtypeStruct((1, feat), f32),
        ),
        in_specs=[smem_spec(), smem_spec()] + [vmem_spec()] * 7,
        out_specs=(vmem_spec(),) * 2,
        scratch_shapes=[pltpu.VMEM(table.shape, f32)],
        compiler_params=limits(6),
        name="input_grads",
    )(in_hbm(groups), coords, tokens, cotangent, gain, table, grad, mine, came)


def branch_kernel(tokens, running, quad, own, *refs):
    came, (out, running_new) = refs[:-2], refs[-2:]
    total = own[...]
    for ref in came:
        total = total + ref[...].astype(f32)
    out[...] = (tokens[...].astype(f32) + total.T).astype(bf16)
    mean = jnp.sum(quad[...], axis=0, keepdims=True) / quad.shape[0]
    running_new[...] = (1.0 - MOMENTUM) * running[...] + MOMENTUM * mean


def branch_out(tokens, running, quad, own, came):
    return pl.pallas_call(
        branch_kernel,
        out_shape=(
            jax.ShapeDtypeStruct(tokens.shape, bf16),
            jax.ShapeDtypeStruct(running.shape, f32),
        ),
        in_specs=[vmem_spec()] * (4 + len(came)),
        out_specs=(vmem_spec(),) * 2,
        compiler_params=limits(6),
        name="branch_out",
    )(tokens, in_hbm(running), quad, own, *came)


def limits(mib):
    return pltpu.CompilerParams(vmem_limit_bytes=mib << 20)


def places(coords):
    return feature_blocks(coords, 0) + feature_blocks(coords, 1)


def cotangent_kernel(coords, *refs):
    pieces, (out, turned) = refs[:-2], refs[-2:]
    rows, width = out.shape[0], pieces[0].shape[1]
    for place, piece in zip(places(coords), pieces):
        first = pl.multiple_of(place * width, width)
        value = piece[rows:, :]
        out[:, pl.ds(first, width)] = value
        turned[pl.ds(first, width), :] = value.T


def normalize_kernel(groups, coords, gain, *refs):
    ins, (out, turned) = refs[:-2], refs[-2:]
    pieces, tables = ins[: len(ins) // 2], ins[len(ins) // 2 :]
    rows, width = out.shape[0], pieces[0].shape[1]
    for place, piece, table in zip(places(coords), pieces, tables):
        first = pl.multiple_of(place * width, width)
        gain_row = gain[:, pl.ds(first, width)]
        for b in range(rows // BLK):
            block = slice(b * BLK, (b + 1) * BLK)
            normed = piece[block, :].astype(f32) * table[pl.ds(groups[b], 1), :]
            out[block, pl.ds(first, width)] = (gain_row * normed).astype(bf16)
        turned[pl.ds(first, width), :] = out[:, pl.ds(first, width)].T


def assembled_shapes(pieces):
    rows, width = pieces[0].shape[0] // 2, pieces[0].shape[1] * len(pieces)
    return (jax.ShapeDtypeStruct((rows, width), bf16), jax.ShapeDtypeStruct((width, rows), bf16))


def cotangent_whole(coords, pieces):
    return pl.pallas_call(
        cotangent_kernel,
        out_shape=assembled_shapes(pieces),
        in_specs=[smem_spec()] + [vmem_spec()] * len(pieces),
        out_specs=(vmem_spec(), vmem_spec()),
        compiler_params=limits(12),
        name="cotangent_whole",
    )(coords, *pieces)


def normalized_whole(groups, coords, gain, pieces, tables):
    return pl.pallas_call(
        normalize_kernel,
        out_shape=assembled_shapes(pieces),
        in_specs=[smem_spec(), smem_spec()] + [vmem_spec()] * (1 + 2 * len(pieces)),
        out_specs=(vmem_spec(), vmem_spec()),
        compiler_params=limits(12),
        name="normalized_whole",
    )(in_hbm(groups), coords, gain, *pieces, *tables)


def rows_product(blocks, turned, right, send, keep, first):
    columns = slice(first, first + right.shape[1])
    half = len(blocks) // 2
    for part, out in ((blocks[:half], send), (blocks[half:], keep)):
        left = jnp.concatenate(
            [turned[pl.ds(pl.multiple_of(b * 128, 128), 128), :] for b in part], axis=0
        )
        out[:, columns] = jnp.dot(left, right, preferred_element_type=f32).astype(out.dtype)


def hidden_kernel(p, lent):
    def kernel(coords, hid, hid_t, dy, dy_t, gate_w, up_w, down_w, hidden_t, ggi_t, gl_t, *outs):
        gate = jnp.dot(hid[...], gate_w[...], preferred_element_type=f32)
        lift = jnp.dot(hid[...], up_w[...], preferred_element_type=f32)
        grad = jnp.dot(dy[...], down_w[...], preferred_element_type=f32)
        sigma = jax.nn.sigmoid(gate)
        act = gate * sigma
        hidden = (act * lift).astype(bf16)
        ggi = (grad * lift * sigma * (1.0 + gate * (1.0 - sigma))).astype(bf16)
        gl = (grad * act).astype(bf16)
        own = row_blocks(coords, PATTERNS[p])
        rows_product(own, dy_t, hidden[:, lent:], outs[0], outs[1], 0)
        both = jnp.concatenate([ggi, gl], axis=1)
        rows_product(own, hid_t, both, outs[0], outs[1], hidden.shape[1] - lent)
        if lent:
            rows_product(row_blocks(coords, PATTERNS[0]), dy_t, hidden[:, :lent], outs[2], outs[3], 0)
        hidden_t[...] = hidden.T
        ggi_t[...] = ggi.T
        gl_t[...] = gl.T

    return kernel


def hidden_part(p, coords, hid, hid_t, dy, dy_t, gate_w, up_w, down_w):
    rows, width = hid.shape
    part = gate_w.shape[1] // RING
    lent = LENT if p == RING - 1 else 0

    def fixed(*shape):
        return pl.BlockSpec(shape, lambda i: (0, 0))

    weight = pl.BlockSpec((width, part), lambda i: (0, p))
    halves = [3 * part - lent] * 2 + ([lent] * 2 if lent else [])
    shapes = [(part, rows)] * 3 + [(width // 2, n) for n in halves]
    return pl.pallas_call(
        hidden_kernel(p, lent),
        grid=(1,),
        out_shape=tuple(jax.ShapeDtypeStruct(shape, bf16) for shape in shapes),
        in_specs=[
            smem_spec(),
            fixed(rows, width),
            fixed(width, rows),
            fixed(rows, width),
            fixed(width, rows),
            weight,
            weight,
            weight,
        ],
        out_specs=tuple(fixed(*shape) for shape in shapes),
        compiler_params=limits(20),
        name="hidden_part",
    )(coords, hid, hid_t, dy, dy_t, gate_w, up_w, down_w)


def back_kernel(pairs):
    def kernel(coords, *refs):
        acts = refs[: pairs * RING]
        weights = refs[pairs * RING : pairs * RING + pairs]
        outs = refs[pairs * RING + pairs :]
        feat = outs[0].shape[1]
        for other, out in ((1, outs[0]), (0, outs[1])):
            total = None
            for j in range(pairs):
                act = jnp.concatenate([r[...] for r in acts[j * RING : (j + 1) * RING]], axis=0)
                left = jnp.concatenate(
                    [
                        weights[j][pl.ds(pl.multiple_of(b * feat, feat), feat), :]
                        for b in feature_blocks(coords, other)
                    ],
                    axis=0,
                )
                term = jnp.dot(left, act, preferred_element_type=f32)
                total = term if total is None else total + term
            for k in range(RING):
                out[k] = total[k * feat : (k + 1) * feat, :].astype(bf16)

    return kernel


def back(coords, acts, weights):
    rows = acts[0][0].shape[1]
    feat = weights[0].shape[0] // (2 * RING)
    pairs = len(weights)
    out = jax.ShapeDtypeStruct((RING, feat, rows), bf16)
    return pl.pallas_call(
        back_kernel(pairs),
        in_specs=[smem_spec()] + [vmem_spec()] * (pairs * RING + pairs),
        out_specs=(vmem_spec(), vmem_spec()),
        out_shape=(out, out),
        compiler_params=limits(20),
        name="back",
    )(coords, *[a for group in acts for a in group], *weights)


def chip_sum_kernel(near, other, own, *sends):
    own[...] = near[0].astype(f32) + other[0].astype(f32)
    for k, send in enumerate(sends, 1):
        send[...] = (near[k].astype(f32) + other[k].astype(f32)).astype(bf16)


def mp_scattered(far, near):
    other = lax.ppermute(far, "c", CORES)
    piece = near.shape[1:]
    own, *sends = pl.pallas_call(
        chip_sum_kernel,
        out_shape=(jax.ShapeDtypeStruct(piece, f32),)
        + (jax.ShapeDtypeStruct(piece, bf16),) * (RING - 1),
        in_specs=[vmem_spec()] * 2,
        out_specs=(vmem_spec(),) * RING,
        compiler_params=limits(6),
        name="chip_sum",
    )(near, other)
    came = []
    for k in (1, 3, 2):
        came.append(lax.ppermute(sends[k - 1], "y", shift(k)))
    return own, came


def split_kernel(*refs):
    ins, (send, kept) = refs[:-2], refs[-2:]
    half = send.shape[0]
    first = 0
    for keep, came in zip(ins[::2], ins[1::2]):
        columns = slice(first, first + keep.shape[1])
        send[:, columns] = (keep[:half, :].astype(f32) + came[:half, :].astype(f32)).astype(bf16)
        kept[:, columns] = (keep[half:, :].astype(f32) + came[half:, :].astype(f32)).astype(bf16)
        first += keep.shape[1]


def split_add(*pairs):
    rows = pairs[0].shape[0] // 2
    half = jax.ShapeDtypeStruct((rows, sum(a.shape[1] for a in pairs[::2])), bf16)
    return pl.pallas_call(
        split_kernel,
        out_shape=(half, half),
        in_specs=[vmem_spec()] * len(pairs),
        out_specs=(vmem_spec(),) * 2,
        compiler_params=limits(8),
        name="split_add",
    )(*pairs)


def sections(part):
    runs = []
    for p in range(RING):
        lent = LENT if p == RING - 1 else 0
        runs.append([(0, p * part + lent, part - lent), (1, p * part, part), (2, p * part, part)])
    runs[0].append((0, (RING - 1) * part, LENT))
    return runs


def finish_kernel(*refs):
    ins, outs = refs[: 2 * RING], refs[2 * RING :]
    for p, runs in enumerate(sections(outs[0].shape[1] // RING)):
        total = ins[2 * p][...].astype(f32) + ins[2 * p + 1][...].astype(f32)
        first = 0
        for out, column, width in runs:
            outs[out][:, column : column + width] = total[:, first : first + width]
            first += width


def finished(pairs, width):
    rows = pairs[0][0].shape[0]
    out = jax.ShapeDtypeStruct((rows, width), f32)
    return pl.pallas_call(
        finish_kernel,
        out_shape=(out,) * 3,
        in_specs=[vmem_spec()] * (2 * RING),
        out_specs=(vmem_spec(),) * 3,
        compiler_params=limits(6),
        name="finished",
    )(*[a for pair in pairs for a in pair])


def body(tokens, norm_gain, running_sq, gate_weight, up_weight, down_weight_t, groups, cotangent):
    tok_rows, feat = tokens.shape
    groups_total = tok_rows * RING * RING // GHOST
    coords = jnp.stack([lax.axis_index(a) for a in ("z", "x", "y", "c")]).astype(jnp.int32)
    gain = norm_gain.reshape(1, -1)
    local, both = stats(groups, coords, tokens, cotangent, groups_total)
    pieces = gathered(both)
    sums = ring_pieces(ring_sum(local, "z"), "x")
    table, quad = scale_table(sums)
    tables = gathered(table)
    (down_weight_t,) = staged(down_weight_t)
    gate_weight, up_weight = staged(gate_weight, up_weight)
    dy_full, dy_turned = cotangent_whole(coords, pieces)
    hid_full, hid_turned = normalized_whole(groups, coords, gain, pieces, tables)
    parts = []
    for p in range(RING):
        parts.append(
            hidden_part(
                p, coords, hid_full, hid_turned, dy_full, dy_turned, gate_weight, up_weight, down_weight_t
            )
        )
    last = []
    for p, (major, first) in enumerate(PATTERNS):
        minor = "x" if major == "z" else "z"
        pair = (NEAR, FAR) if first == 0 else (FAR, NEAR)
        send, keep = parts[p][3:5]
        for i, (axis, route) in enumerate(((major, 0), (major, 1), (minor, 0), (minor, 1)), 1):
            came = lax.ppermute(send, axis, pair[route])
            if i < 4:
                more = ()
                if i == 1 and p == 0:
                    more = (parts[-1][6], lax.ppermute(parts[-1][5], axis, pair[route]))
                send, keep = split_add(keep, came, *more)
        last.append((keep, came))
    grad_down_t, grad_gate, grad_up = finished(last, gate_weight.shape[1])

    far, near = back(
        coords, [[q[1] for q in parts], [q[2] for q in parts]], [gate_weight, up_weight]
    )
    kept, came = mp_scattered(far, near)
    grad, local = partials(groups, tokens, table, kept, came)
    mine, came = tok_halves(local)
    grad_tokens, grad_gain = input_grads(groups, coords, tokens, cotangent, gain, table, grad, mine, came)

    far, near = back(coords, [[q[0] for q in parts]], [down_weight_t])
    kept, came = mp_scattered(far, near)
    block_out, running_new = branch_out(tokens, running_sq.reshape(1, feat), quad, kept, came)
    return (
        block_out,
        grad_tokens,
        running_new.reshape(feat),
        grad_gain.reshape(feat),
        grad_gate,
        grad_up,
        grad_down_t,
    )


def solution(mesh):
    torus = Mesh(mesh.devices.reshape(RING, RING, RING, 2), ("z", "x", "y", "c"))
    tok, mp = ("z", "x"), ("y", "c")
    placed = (P(tok, mp), P(), P(mp), P(None, mp), P(None, mp), P(None, mp), P(tok), P(tok, mp))
    out = (P(tok, mp), P(tok, mp), P(mp), P(mp), P(tok, mp), P(tok, mp), P(tok, mp))

    return jax.shard_map(body, mesh=torus, in_specs=placed, out_specs=out, check_vma=False)
```

```python
import jax
import jax.numpy as jnp
from jax import lax
from jax.experimental import pallas as pl
from jax.experimental.pallas import tpu as pltpu
from jax.sharding import Mesh
from jax.sharding import PartitionSpec as P


GHOST = 128
BLK = 16
RING = 4
NEAR = [(i, i ^ 1) for i in range(RING)]
FAR = [(i, RING - 1 - i) for i in range(RING)]
CORES = [(0, 1), (1, 0)]
EPSILON = 1e-05
MOMENTUM = 0.1


bf16 = jnp.bfloat16
f32 = jnp.float32


PATTERNS = (("z", 0), ("z", 1), ("x", 0), ("x", 1))
LENT = 128


def halving(i, first):
    near, far = i ^ 1, RING - 1 - i
    p, q = (near, far) if first == 0 else (far, near)
    return [RING - 1 - p if first == 0 else p ^ 1, p, q, i]


def row_blocks(coords, pattern):
    major, first = pattern
    hz, hx = halving(coords[0], first), halving(coords[1], first)
    if major == "z":
        return [RING * a + b for a in hz for b in hx]
    return [RING * a + b for b in hx for a in hz]


def feature_blocks(coords, other):
    core = coords[3] if other == 0 else 1 - coords[3]
    return [2 * ((coords[2] + k) & (RING - 1)) + core for k in range(RING)]


def shift(k):
    return [(i, (i + k) % RING) for i in range(RING)]


def vmem_spec():
    return pl.BlockSpec(memory_space=pltpu.VMEM)


def smem_spec():
    return pl.BlockSpec(memory_space=pltpu.SMEM)


def in_hbm(x):
    return pltpu.with_memory_space_constraint(x, pltpu.HBM)


def gathered(x):
    near = [x]
    for k in (1, 3, 2):
        near.append(lax.ppermute(x, "y", shift(-k)))
    near = [near[0], near[1], near[3], near[2]]
    far = []
    for k in range(RING):
        far.append(lax.ppermute(near[k], "c", CORES))
    return near + far


def block_sum(value):
    return jnp.sum(value, axis=0, keepdims=True)


def own_gain(coords, gain, feat):
    return gain[:, pl.ds(pl.multiple_of((2 * coords[2] + coords[3]) * feat, feat), feat)]


def add_kernel(left, right, out):
    out[...] = left[...] + right[...]


def pair_added(left, right):
    return pl.pallas_call(
        add_kernel,
        out_shape=jax.ShapeDtypeStruct(left.shape, left.dtype),
        in_specs=[vmem_spec()] * 2,
        out_specs=vmem_spec(),
        compiler_params=limits(1),
        name="pair_added",
    )(left, right)


def tok_halves(x):
    for i, (axis, pairs) in enumerate((("z", NEAR), ("z", FAR), ("x", NEAR), ("x", FAR)), 1):
        came = lax.ppermute(x, axis, pairs)
        if i < 4:
            x = pair_added(x, came)
    return x, came


def ring_sum_kernel(*refs):
    ins, out = refs[:-1], refs[-1]
    out[...] = (ins[0][...] + ins[3][...]) + (ins[1][...] + ins[2][...])


def ring_pieces(x, axis):
    came = [x]
    for k in (1, 3, 2):
        came.append(lax.ppermute(x, axis, shift(k)))
    return came


def ring_sum(x, axis):
    pieces = ring_pieces(x, axis)
    return pl.pallas_call(
        ring_sum_kernel,
        out_shape=jax.ShapeDtypeStruct(x.shape, x.dtype),
        in_specs=[vmem_spec()] * RING,
        out_specs=vmem_spec(),
        compiler_params=limits(1),
        name="ring_sum",
    )(*pieces)


STAGE_CUTS = 4


def stage_kernel(*refs):
    count = (len(refs) - 1) // 2
    sems = refs[-1]
    copies = []
    for i in range(count):
        source, out = refs[i], refs[count + i]
        rows = source.shape[0] // STAGE_CUTS
        for j in range(STAGE_CUTS):
            part = pl.ds(j * rows, rows)
            copies.append(
                pltpu.make_async_copy(source.at[part], out.at[part], sems.at[i * STAGE_CUTS + j])
            )
    for copy in copies:
        copy.start()
    for copy in copies:
        copy.wait()


def staged(*weights):
    return pl.pallas_call(
        stage_kernel,
        out_shape=tuple(pltpu.VMEM(w.shape, w.dtype) for w in weights),
        in_specs=[pl.BlockSpec(memory_space=pltpu.HBM)] * len(weights),
        out_specs=(vmem_spec(),) * len(weights),
        scratch_shapes=[pltpu.SemaphoreType.DMA((STAGE_CUTS * len(weights),))],
        compiler_params=limits(1),
        name="staged",
    )(*[in_hbm(w) for w in weights])


def stats_kernel(groups, coords, tokens, cotangent, out, both):
    rows = tokens.shape[0]
    both[:rows, :] = tokens[...]
    both[rows:, :] = cotangent[...]
    out[...] = jnp.zeros_like(out)
    for b in range(rows // BLK):
        value = tokens[b * BLK : (b + 1) * BLK, :].astype(f32)
        row = pl.ds(groups[b], 1)
        out[row, :] = out[row, :] + block_sum(value * value)


def stats(groups, coords, tokens, cotangent, groups_total):
    rows, feat = tokens.shape
    return pl.pallas_call(
        stats_kernel,
        out_shape=(
            jax.ShapeDtypeStruct((groups_total, feat), f32),
            jax.ShapeDtypeStruct((2 * rows, feat), bf16),
        ),
        in_specs=[smem_spec(), smem_spec(), vmem_spec(), vmem_spec()],
        out_specs=(vmem_spec(),) * 2,
        compiler_params=limits(4),
        name="stats",
    )(in_hbm(groups), coords, in_hbm(tokens), in_hbm(cotangent))


def table_kernel(a, b, c, d, table, quad):
    quad_mean = ((a[...] + d[...]) + (b[...] + c[...])) * (1.0 / GHOST)
    quad[...] = quad_mean
    table[...] = lax.rsqrt(quad_mean + EPSILON)


def scale_table(pieces):
    out = jax.ShapeDtypeStruct(pieces[0].shape, f32)
    return pl.pallas_call(
        table_kernel,
        out_shape=(out, out),
        in_specs=[vmem_spec()] * RING,
        out_specs=(vmem_spec(),) * 2,
        compiler_params=limits(2),
        name="scale_table",
    )(*pieces)


def partial_kernel(groups, tokens, table, own, *refs):
    came, (grad, out) = refs[:-2], refs[-2:]
    feat = tokens.shape[1]
    total = own[:feat, :]
    for ref in came:
        total = total + ref[:feat, :].astype(f32)
    grad[...] = total.T
    out[...] = jnp.zeros_like(out)
    for b in range(tokens.shape[0] // BLK):
        rows = slice(b * BLK, (b + 1) * BLK)
        row = pl.ds(groups[b], 1)
        normed = tokens[rows, :].astype(f32) * table[row, :]
        out[row, :] = out[row, :] + block_sum(grad[rows, :] * normed)


def partials(groups, tokens, table, own, came):
    rows, feat = tokens.shape
    return pl.pallas_call(
        partial_kernel,
        out_shape=(
            jax.ShapeDtypeStruct((rows, feat), f32),
            jax.ShapeDtypeStruct(table.shape, f32),
        ),
        in_specs=[smem_spec()] + [vmem_spec()] * (3 + len(came)),
        out_specs=(vmem_spec(),) * 2,
        compiler_params=limits(6),
        name="partials",
    )(in_hbm(groups), tokens, table, own, *came)


def input_kernel(groups, coords, tokens, cotangent, gain, table, grad, mine, came, out, grad_gain, acc):
    partial = mine[...] + came[...]
    grad_gain[...] = jnp.sum(partial, axis=0, keepdims=True)
    gain_row = own_gain(coords, gain, tokens.shape[1])
    acc[...] = gain_row * partial * (1.0 / GHOST)
    for b in range(tokens.shape[0] // BLK):
        rows = slice(b * BLK, (b + 1) * BLK)
        row = pl.ds(groups[b], 1)
        scale = table[row, :]
        normed = tokens[rows, :].astype(f32) * scale
        inner = gain_row * grad[rows, :] - normed * acc[row, :]
        out[rows, :] = (cotangent[rows, :].astype(f32) + scale * inner).astype(bf16)


def input_grads(groups, coords, tokens, cotangent, gain, table, grad, mine, came):
    rows, feat = tokens.shape
    return pl.pallas_call(
        input_kernel,
        out_shape=(
            jax.ShapeDtypeStruct((rows, feat), bf16),
            jax.ShapeDtypeStruct((1, feat), f32),
        ),
        in_specs=[smem_spec(), smem_spec()] + [vmem_spec()] * 7,
        out_specs=(vmem_spec(),) * 2,
        scratch_shapes=[pltpu.VMEM(table.shape, f32)],
        compiler_params=limits(6),
        name="input_grads",
    )(in_hbm(groups), coords, tokens, cotangent, gain, table, grad, mine, came)


def branch_kernel(tokens, running, quad, own, *refs):
    came, (out, running_new) = refs[:-2], refs[-2:]
    feat = tokens.shape[1]
    total = own[feat:, :]
    for ref in came:
        total = total + ref[feat:, :].astype(f32)
    out[...] = (tokens[...].astype(f32) + total.T).astype(bf16)
    mean = jnp.sum(quad[...], axis=0, keepdims=True) / quad.shape[0]
    running_new[...] = (1.0 - MOMENTUM) * running[...] + MOMENTUM * mean


def branch_out(tokens, running, quad, own, came):
    return pl.pallas_call(
        branch_kernel,
        out_shape=(
            jax.ShapeDtypeStruct(tokens.shape, bf16),
            jax.ShapeDtypeStruct(running.shape, f32),
        ),
        in_specs=[vmem_spec()] * (4 + len(came)),
        out_specs=(vmem_spec(),) * 2,
        compiler_params=limits(6),
        name="branch_out",
    )(tokens, in_hbm(running), quad, own, *came)


def limits(mib):
    return pltpu.CompilerParams(vmem_limit_bytes=mib << 20)


def places(coords):
    return feature_blocks(coords, 0) + feature_blocks(coords, 1)


def cotangent_kernel(coords, *refs):
    pieces, (out, turned) = refs[:-2], refs[-2:]
    rows, width = out.shape[0], pieces[0].shape[1]
    for place, piece in zip(places(coords), pieces):
        first = pl.multiple_of(place * width, width)
        value = piece[rows:, :]
        out[:, pl.ds(first, width)] = value
        turned[pl.ds(first, width), :] = value.T


def normalize_kernel(groups, coords, gain, *refs):
    ins, (out, turned) = refs[:-2], refs[-2:]
    pieces, tables = ins[: len(ins) // 2], ins[len(ins) // 2 :]
    rows, width = out.shape[0], pieces[0].shape[1]
    for place, piece, table in zip(places(coords), pieces, tables):
        first = pl.multiple_of(place * width, width)
        gain_row = gain[:, pl.ds(first, width)]
        for b in range(rows // BLK):
            block = slice(b * BLK, (b + 1) * BLK)
            normed = piece[block, :].astype(f32) * table[pl.ds(groups[b], 1), :]
            out[block, pl.ds(first, width)] = (gain_row * normed).astype(bf16)
        turned[pl.ds(first, width), :] = out[:, pl.ds(first, width)].T


def assembled_shapes(pieces):
    rows, width = pieces[0].shape[0] // 2, pieces[0].shape[1] * len(pieces)
    return (jax.ShapeDtypeStruct((rows, width), bf16), jax.ShapeDtypeStruct((width, rows), bf16))


def cotangent_whole(coords, pieces):
    return pl.pallas_call(
        cotangent_kernel,
        out_shape=assembled_shapes(pieces),
        in_specs=[smem_spec()] + [vmem_spec()] * len(pieces),
        out_specs=(vmem_spec(), vmem_spec()),
        compiler_params=limits(12),
        name="cotangent_whole",
    )(coords, *pieces)


def normalized_whole(groups, coords, gain, pieces, tables):
    return pl.pallas_call(
        normalize_kernel,
        out_shape=assembled_shapes(pieces),
        in_specs=[smem_spec(), smem_spec()] + [vmem_spec()] * (1 + 2 * len(pieces)),
        out_specs=(vmem_spec(), vmem_spec()),
        compiler_params=limits(12),
        name="normalized_whole",
    )(in_hbm(groups), coords, gain, *pieces, *tables)


def rows_product(blocks, turned, right, outs, first):
    columns = slice(first, first + right.shape[1])
    half = len(blocks) // 2
    values = []
    for part in (blocks[:half], blocks[half:]):
        left = jnp.concatenate(
            [turned[pl.ds(pl.multiple_of(b * 128, 128), 128), :] for b in part], axis=0
        )
        values.append(jnp.dot(left, right, preferred_element_type=f32).astype(bf16))
    done = 0
    for out in outs:
        value, start = values[done // values[0].shape[0]], done % values[0].shape[0]
        out[:, columns] = value[start : start + out.shape[0], :]
        done += out.shape[0]


def hidden_kernel(p, lent):
    def kernel(coords, hid, hid_t, dy, dy_t, gate_w, up_w, down_w, hidden_t, ggi_t, gl_t, *outs):
        gate = jnp.dot(hid[...], gate_w[...], preferred_element_type=f32)
        lift = jnp.dot(hid[...], up_w[...], preferred_element_type=f32)
        grad = jnp.dot(dy[...], down_w[...], preferred_element_type=f32)
        sigma = jax.nn.sigmoid(gate)
        act = gate * sigma
        hidden = (act * lift).astype(bf16)
        ggi = (grad * lift * sigma * (1.0 + gate * (1.0 - sigma))).astype(bf16)
        gl = (grad * act).astype(bf16)
        own = row_blocks(coords, PATTERNS[p])
        rows_product(own, dy_t, hidden[:, lent:], outs[:3], 0)
        both = jnp.concatenate([ggi, gl], axis=1)
        rows_product(own, hid_t, both, outs[:3], hidden.shape[1] - lent)
        if lent:
            rows_product(row_blocks(coords, PATTERNS[0]), dy_t, hidden[:, :lent], outs[3:], 0)
        hidden_t[...] = hidden.T
        ggi_t[...] = ggi.T
        gl_t[...] = gl.T

    return kernel


def hidden_part(p, coords, hid, hid_t, dy, dy_t, gate_w, up_w, down_w):
    rows, width = hid.shape
    part = gate_w.shape[1] // RING
    lent = LENT if p == RING - 1 else 0

    def fixed(*shape):
        return pl.BlockSpec(shape, lambda i: (0, 0))

    weight = pl.BlockSpec((width, part), lambda i: (0, p))
    columns = 3 * part - lent
    shapes = [(part, rows)] * 3 + [(width // 4, columns)] * 2 + [(width // 2, columns)]
    shapes += [(width // 2, lent)] * 2 if lent else []
    return pl.pallas_call(
        hidden_kernel(p, lent),
        grid=(1,),
        out_shape=tuple(jax.ShapeDtypeStruct(shape, bf16) for shape in shapes),
        in_specs=[
            smem_spec(),
            fixed(rows, width),
            fixed(width, rows),
            fixed(rows, width),
            fixed(width, rows),
            weight,
            weight,
            weight,
        ],
        out_specs=tuple(fixed(*shape) for shape in shapes),
        compiler_params=limits(20),
        name="hidden_part",
    )(coords, hid, hid_t, dy, dy_t, gate_w, up_w, down_w)


def back_kernel(coords, *refs):
    acts, weights, outs = refs[: 3 * RING], refs[3 * RING : 3 * RING + 3], refs[3 * RING + 3 :]
    feat = outs[0].shape[1]
    whole = [
        jnp.concatenate([r[...] for r in acts[j * RING : (j + 1) * RING]], axis=0) for j in range(3)
    ]
    for other, out in ((1, outs[0]), (0, outs[1])):
        terms = []
        for weight, act in zip(weights, whole):
            left = jnp.concatenate(
                [
                    weight[pl.ds(pl.multiple_of(b * feat, feat), feat), :]
                    for b in feature_blocks(coords, other)
                ],
                axis=0,
            )
            terms.append(jnp.dot(left, act, preferred_element_type=f32))
        for j, total in enumerate((terms[0] + terms[1], terms[2])):
            for k in range(RING):
                out[j * RING + k] = total[k * feat : (k + 1) * feat, :].astype(bf16)


def back(coords, acts, weights):
    rows = acts[0][0].shape[1]
    feat = weights[0].shape[0] // (2 * RING)
    out = jax.ShapeDtypeStruct((2 * RING, feat, rows), bf16)
    return pl.pallas_call(
        back_kernel,
        in_specs=[smem_spec()] + [vmem_spec()] * (3 * RING + 3),
        out_specs=(vmem_spec(), vmem_spec()),
        out_shape=(out, out),
        compiler_params=limits(24),
        name="back",
    )(coords, *[a for group in acts for a in group], *weights)


def chip_sum_kernel(near, other, own, *sends):
    feat = near.shape[1]
    for j in range(2):
        rows = slice(j * feat, (j + 1) * feat)
        own[rows, :] = near[j * RING].astype(f32) + other[j * RING].astype(f32)
        for k, send in enumerate(sends, 1):
            i = j * RING + k
            send[rows, :] = (near[i].astype(f32) + other[i].astype(f32)).astype(bf16)


def mp_scattered(far, near):
    other = lax.ppermute(far, "c", CORES)
    piece = (2 * near.shape[1], near.shape[2])
    own, *sends = pl.pallas_call(
        chip_sum_kernel,
        out_shape=(jax.ShapeDtypeStruct(piece, f32),)
        + (jax.ShapeDtypeStruct(piece, bf16),) * (RING - 1),
        in_specs=[vmem_spec()] * 2,
        out_specs=(vmem_spec(),) * RING,
        compiler_params=limits(8),
        name="chip_sum",
    )(near, other)
    came = []
    for k in (1, 3, 2):
        came.append(lax.ppermute(sends[k - 1], "y", shift(k)))
    return own, came


def split_kernel(*refs):
    ins, (send, kept) = refs[:-2], refs[-2:]
    half = send.shape[0]
    first = 0
    for keep, came in zip(ins[::2], ins[1::2]):
        columns = slice(first, first + keep.shape[1])
        send[:, columns] = (keep[:half, :].astype(f32) + came[:half, :].astype(f32)).astype(bf16)
        kept[:, columns] = (keep[half:, :].astype(f32) + came[half:, :].astype(f32)).astype(bf16)
        first += keep.shape[1]


def split_add(*pairs):
    rows = pairs[0].shape[0] // 2
    half = jax.ShapeDtypeStruct((rows, sum(a.shape[1] for a in pairs[::2])), bf16)
    return pl.pallas_call(
        split_kernel,
        out_shape=(half, half),
        in_specs=[vmem_spec()] * len(pairs),
        out_specs=(vmem_spec(),) * 2,
        compiler_params=limits(8),
        name="split_add",
    )(*pairs)


def half_kernel(half):
    def kernel(*refs):
        ins, out = refs[:-1], refs[-1]
        rows = out.shape[0]
        first = 0
        for keep, came in zip(ins[::2], ins[1::2]):
            mine = keep[half * rows : (half + 1) * rows, :]
            start = half * rows if came.shape[0] > rows else 0
            theirs = came[start : start + rows, :]
            columns = slice(first, first + keep.shape[1])
            out[:, columns] = (mine.astype(f32) + theirs.astype(f32)).astype(bf16)
            first += keep.shape[1]

    return kernel


def half_add(half, *pairs):
    out = jax.ShapeDtypeStruct((pairs[0].shape[0] // 2, sum(a.shape[1] for a in pairs[::2])), bf16)
    return pl.pallas_call(
        half_kernel(half),
        out_shape=out,
        in_specs=[vmem_spec()] * len(pairs),
        out_specs=vmem_spec(),
        compiler_params=limits(6),
        name="half_add",
    )(*pairs)


def sections(part):
    runs = []
    for p in range(RING):
        lent = LENT if p == RING - 1 else 0
        runs.append([(0, p * part + lent, part - lent), (1, p * part, part), (2, p * part, part)])
    runs[0].append((0, (RING - 1) * part, LENT))
    return runs


def finish_kernel(*refs):
    ins, outs = refs[: 2 * RING], refs[2 * RING :]
    for p, runs in enumerate(sections(outs[0].shape[1] // RING)):
        total = ins[2 * p][...].astype(f32) + ins[2 * p + 1][...].astype(f32)
        first = 0
        for out, column, width in runs:
            outs[out][:, column : column + width] = total[:, first : first + width]
            first += width


def finished(pairs, width):
    rows = pairs[0][0].shape[0]
    out = jax.ShapeDtypeStruct((rows, width), f32)
    return pl.pallas_call(
        finish_kernel,
        out_shape=(out,) * 3,
        in_specs=[vmem_spec()] * (2 * RING),
        out_specs=(vmem_spec(),) * 3,
        compiler_params=limits(6),
        name="finished",
    )(*[a for pair in pairs for a in pair])


def body(tokens, norm_gain, running_sq, gate_weight, up_weight, down_weight_t, groups, cotangent):
    tok_rows, feat = tokens.shape
    groups_total = tok_rows * RING * RING // GHOST
    coords = jnp.stack([lax.axis_index(a) for a in ("z", "x", "y", "c")]).astype(jnp.int32)
    gain = norm_gain.reshape(1, -1)
    local, both = stats(groups, coords, tokens, cotangent, groups_total)
    pieces = gathered(both)
    sums = ring_pieces(ring_sum(local, "z"), "x")
    table, quad = scale_table(sums)
    tables = gathered(table)
    (down_weight_t,) = staged(down_weight_t)
    gate_weight, up_weight = staged(gate_weight, up_weight)
    dy_full, dy_turned = cotangent_whole(coords, pieces)
    hid_full, hid_turned = normalized_whole(groups, coords, gain, pieces, tables)
    parts = []
    for p in range(RING):
        parts.append(
            hidden_part(
                p, coords, hid_full, hid_turned, dy_full, dy_turned, gate_weight, up_weight, down_weight_t
            )
        )
    last = []
    for p, (major, first) in enumerate(PATTERNS):
        minor = "x" if major == "z" else "z"
        pair = (NEAR, FAR) if first == 0 else (FAR, NEAR)
        send_a, send_b, keep = parts[p][3:6]
        more = ()
        if p == 0:
            more = (parts[-1][7], lax.ppermute(parts[-1][6], major, pair[0]))
        came_a = lax.ppermute(send_a, major, pair[0])
        came_b = lax.ppermute(send_b, major, pair[0])
        send = half_add(0, keep, came_a, *more)
        came = lax.ppermute(send, major, pair[1])
        keep = half_add(1, keep, came_b, *more)
        for route in (0, 1):
            send, keep = split_add(keep, came)
            came = lax.ppermute(send, minor, pair[route])
        last.append((keep, came))
    grad_down_t, grad_gate, grad_up = finished(last, gate_weight.shape[1])

    far, near = back(
        coords,
        [[q[1] for q in parts], [q[2] for q in parts], [q[0] for q in parts]],
        [gate_weight, up_weight, down_weight_t],
    )
    kept, came_y = mp_scattered(far, near)
    grad, local = partials(groups, tokens, table, kept, came_y)
    mine, came = tok_halves(local)
    grad_tokens, grad_gain = input_grads(groups, coords, tokens, cotangent, gain, table, grad, mine, came)

    block_out, running_new = branch_out(tokens, running_sq.reshape(1, feat), quad, kept, came_y)
    return (
        block_out,
        grad_tokens,
        running_new.reshape(feat),
        grad_gain.reshape(feat),
        grad_gate,
        grad_up,
        grad_down_t,
    )


def solution(mesh):
    torus = Mesh(mesh.devices.reshape(RING, RING, RING, 2), ("z", "x", "y", "c"))
    tok, mp = ("z", "x"), ("y", "c")
    placed = (P(tok, mp), P(), P(mp), P(None, mp), P(None, mp), P(None, mp), P(tok), P(tok, mp))
    out = (P(tok, mp), P(tok, mp), P(mp), P(mp), P(tok, mp), P(tok, mp), P(tok, mp))

    return jax.shard_map(body, mesh=torus, in_specs=placed, out_specs=out, check_vma=False)
```

```python
import jax
import jax.numpy as jnp
from jax import lax
from jax.experimental import pallas as pl
from jax.experimental.pallas import tpu as pltpu
from jax.sharding import Mesh
from jax.sharding import PartitionSpec as P


GHOST = 128
BLK = 16
RING = 4
NEAR = [(i, i ^ 1) for i in range(RING)]
FAR = [(i, RING - 1 - i) for i in range(RING)]
CORES = [(0, 1), (1, 0)]
EPSILON = 1e-05
MOMENTUM = 0.1


bf16 = jnp.bfloat16
f32 = jnp.float32


PATTERNS = (("z", 0), ("z", 1), ("x", 0), ("x", 1))
LENT = 128


def halving(i, first):
    near, far = i ^ 1, RING - 1 - i
    p, q = (near, far) if first == 0 else (far, near)
    return [RING - 1 - p if first == 0 else p ^ 1, p, q, i]


def row_blocks(coords, pattern):
    major, first = pattern
    hz, hx = halving(coords[0], first), halving(coords[1], first)
    if major == "z":
        return [RING * a + b for a in hz for b in hx]
    return [RING * a + b for b in hx for a in hz]


def feature_blocks(coords, other):
    core = coords[3] if other == 0 else 1 - coords[3]
    return [2 * ((coords[2] + k) & (RING - 1)) + core for k in range(RING)]


def shift(k):
    return [(i, (i + k) % RING) for i in range(RING)]


def vmem_spec():
    return pl.BlockSpec(memory_space=pltpu.VMEM)


def smem_spec():
    return pl.BlockSpec(memory_space=pltpu.SMEM)


def in_hbm(x):
    return pltpu.with_memory_space_constraint(x, pltpu.HBM)


def gathered(x):
    near = [x]
    for k in (1, 3, 2):
        near.append(lax.ppermute(x, "y", shift(-k)))
    near = [near[0], near[1], near[3], near[2]]
    far = []
    for k in range(RING):
        far.append(lax.ppermute(near[k], "c", CORES))
    return near + far


def block_sum(value):
    return jnp.sum(value, axis=0, keepdims=True)


def own_gain(coords, gain, feat):
    return gain[:, pl.ds(pl.multiple_of((2 * coords[2] + coords[3]) * feat, feat), feat)]


def add_kernel(left, right, out):
    out[...] = left[...] + right[...]


def pair_added(left, right):
    return pl.pallas_call(
        add_kernel,
        out_shape=jax.ShapeDtypeStruct(left.shape, left.dtype),
        in_specs=[vmem_spec()] * 2,
        out_specs=vmem_spec(),
        compiler_params=limits(1),
        name="pair_added",
    )(left, right)


def tok_halves(x):
    for i, (axis, pairs) in enumerate((("z", NEAR), ("z", FAR), ("x", NEAR), ("x", FAR)), 1):
        came = lax.ppermute(x, axis, pairs)
        if i < 4:
            x = pair_added(x, came)
    return x, came


def ring_sum_kernel(*refs):
    ins, out = refs[:-1], refs[-1]
    out[...] = (ins[0][...] + ins[3][...]) + (ins[1][...] + ins[2][...])


def ring_pieces(x, axis):
    came = [x]
    for k in (1, 3, 2):
        came.append(lax.ppermute(x, axis, shift(k)))
    return came


def ring_sum(x, axis):
    pieces = ring_pieces(x, axis)
    return pl.pallas_call(
        ring_sum_kernel,
        out_shape=jax.ShapeDtypeStruct(x.shape, x.dtype),
        in_specs=[vmem_spec()] * RING,
        out_specs=vmem_spec(),
        compiler_params=limits(1),
        name="ring_sum",
    )(*pieces)


STAGE_CUTS = 4


def stage_kernel(*refs):
    count = (len(refs) - 1) // 2
    sems = refs[-1]
    copies = []
    for i in range(count):
        source, out = refs[i], refs[count + i]
        rows = source.shape[0] // STAGE_CUTS
        for j in range(STAGE_CUTS):
            part = pl.ds(j * rows, rows)
            copies.append(
                pltpu.make_async_copy(source.at[part], out.at[part], sems.at[i * STAGE_CUTS + j])
            )
    for copy in copies:
        copy.start()
    for copy in copies:
        copy.wait()


def staged(*weights):
    return pl.pallas_call(
        stage_kernel,
        out_shape=tuple(pltpu.VMEM(w.shape, w.dtype) for w in weights),
        in_specs=[pl.BlockSpec(memory_space=pltpu.HBM)] * len(weights),
        out_specs=(vmem_spec(),) * len(weights),
        scratch_shapes=[pltpu.SemaphoreType.DMA((STAGE_CUTS * len(weights),))],
        compiler_params=limits(1),
        name="staged",
    )(*[in_hbm(w) for w in weights])


def stats_kernel(groups, coords, tokens, cotangent, out, both):
    rows = tokens.shape[0]
    both[:rows, :] = tokens[...]
    both[rows:, :] = cotangent[...]
    out[...] = jnp.zeros_like(out)
    for b in range(rows // BLK):
        value = tokens[b * BLK : (b + 1) * BLK, :].astype(f32)
        row = pl.ds(groups[b], 1)
        out[row, :] = out[row, :] + block_sum(value * value)


def stats(groups, coords, tokens, cotangent, groups_total):
    rows, feat = tokens.shape
    return pl.pallas_call(
        stats_kernel,
        out_shape=(
            jax.ShapeDtypeStruct((groups_total, feat), f32),
            jax.ShapeDtypeStruct((2 * rows, feat), bf16),
        ),
        in_specs=[smem_spec(), smem_spec(), vmem_spec(), vmem_spec()],
        out_specs=(vmem_spec(),) * 2,
        compiler_params=limits(4),
        name="stats",
    )(in_hbm(groups), coords, in_hbm(tokens), in_hbm(cotangent))


def table_kernel(a, b, c, d, table, quad):
    quad_mean = ((a[...] + d[...]) + (b[...] + c[...])) * (1.0 / GHOST)
    quad[...] = quad_mean
    table[...] = lax.rsqrt(quad_mean + EPSILON)


def scale_table(pieces):
    out = jax.ShapeDtypeStruct(pieces[0].shape, f32)
    return pl.pallas_call(
        table_kernel,
        out_shape=(out, out),
        in_specs=[vmem_spec()] * RING,
        out_specs=(vmem_spec(),) * 2,
        compiler_params=limits(2),
        name="scale_table",
    )(*pieces)


def partial_kernel(groups, tokens, table, own, *refs):
    came, (grad, out) = refs[:-2], refs[-2:]
    feat = tokens.shape[1]
    total = own[:feat, :]
    for ref in came:
        total = total + ref[:feat, :].astype(f32)
    grad[...] = total.T
    out[...] = jnp.zeros_like(out)
    for b in range(tokens.shape[0] // BLK):
        rows = slice(b * BLK, (b + 1) * BLK)
        row = pl.ds(groups[b], 1)
        normed = tokens[rows, :].astype(f32) * table[row, :]
        out[row, :] = out[row, :] + block_sum(grad[rows, :] * normed)


def partials(groups, tokens, table, own, came):
    rows, feat = tokens.shape
    return pl.pallas_call(
        partial_kernel,
        out_shape=(
            jax.ShapeDtypeStruct((rows, feat), f32),
            jax.ShapeDtypeStruct(table.shape, f32),
        ),
        in_specs=[smem_spec()] + [vmem_spec()] * (3 + len(came)),
        out_specs=(vmem_spec(),) * 2,
        compiler_params=limits(6),
        name="partials",
    )(in_hbm(groups), tokens, table, own, *came)


def input_kernel(groups, coords, tokens, cotangent, gain, table, grad, mine, came, out, grad_gain, acc):
    partial = mine[...] + came[...]
    grad_gain[...] = jnp.sum(partial, axis=0, keepdims=True)
    gain_row = own_gain(coords, gain, tokens.shape[1])
    acc[...] = gain_row * partial * (1.0 / GHOST)
    for b in range(tokens.shape[0] // BLK):
        rows = slice(b * BLK, (b + 1) * BLK)
        row = pl.ds(groups[b], 1)
        scale = table[row, :]
        normed = tokens[rows, :].astype(f32) * scale
        inner = gain_row * grad[rows, :] - normed * acc[row, :]
        out[rows, :] = (cotangent[rows, :].astype(f32) + scale * inner).astype(bf16)


def input_grads(groups, coords, tokens, cotangent, gain, table, grad, mine, came):
    rows, feat = tokens.shape
    return pl.pallas_call(
        input_kernel,
        out_shape=(
            jax.ShapeDtypeStruct((rows, feat), bf16),
            jax.ShapeDtypeStruct((1, feat), f32),
        ),
        in_specs=[smem_spec(), smem_spec()] + [vmem_spec()] * 7,
        out_specs=(vmem_spec(),) * 2,
        scratch_shapes=[pltpu.VMEM(table.shape, f32)],
        compiler_params=limits(6),
        name="input_grads",
    )(in_hbm(groups), coords, tokens, cotangent, gain, table, grad, mine, came)


def branch_kernel(tokens, running, quad, own, *refs):
    came, (out, running_new) = refs[:-2], refs[-2:]
    feat = tokens.shape[1]
    total = own[feat:, :]
    for ref in came:
        total = total + ref[feat:, :].astype(f32)
    out[...] = (tokens[...].astype(f32) + total.T).astype(bf16)
    mean = jnp.sum(quad[...], axis=0, keepdims=True) / quad.shape[0]
    running_new[...] = (1.0 - MOMENTUM) * running[...] + MOMENTUM * mean


def branch_out(tokens, running, quad, own, came):
    return pl.pallas_call(
        branch_kernel,
        out_shape=(
            jax.ShapeDtypeStruct(tokens.shape, bf16),
            jax.ShapeDtypeStruct(running.shape, f32),
        ),
        in_specs=[vmem_spec()] * (4 + len(came)),
        out_specs=(vmem_spec(),) * 2,
        compiler_params=limits(6),
        name="branch_out",
    )(tokens, in_hbm(running), quad, own, *came)


def limits(mib):
    return pltpu.CompilerParams(vmem_limit_bytes=mib << 20)


def places(coords):
    return feature_blocks(coords, 0) + feature_blocks(coords, 1)


def cotangent_kernel(coords, *refs):
    pieces, (out, turned) = refs[:-2], refs[-2:]
    rows, width = out.shape[0], pieces[0].shape[1]
    for place, piece in zip(places(coords), pieces):
        first = pl.multiple_of(place * width, width)
        value = piece[rows:, :]
        out[:, pl.ds(first, width)] = value
        turned[pl.ds(first, width), :] = value.T


def normalize_kernel(groups, coords, gain, *refs):
    ins, (out, turned) = refs[:-2], refs[-2:]
    pieces, tables = ins[: len(ins) // 2], ins[len(ins) // 2 :]
    rows, width = out.shape[0], pieces[0].shape[1]
    for place, piece, table in zip(places(coords), pieces, tables):
        first = pl.multiple_of(place * width, width)
        gain_row = gain[:, pl.ds(first, width)]
        for b in range(rows // BLK):
            block = slice(b * BLK, (b + 1) * BLK)
            normed = piece[block, :].astype(f32) * table[pl.ds(groups[b], 1), :]
            out[block, pl.ds(first, width)] = (gain_row * normed).astype(bf16)
        turned[pl.ds(first, width), :] = out[:, pl.ds(first, width)].T


def assembled_shapes(pieces):
    rows, width = pieces[0].shape[0] // 2, pieces[0].shape[1] * len(pieces)
    return (jax.ShapeDtypeStruct((rows, width), bf16), jax.ShapeDtypeStruct((width, rows), bf16))


def cotangent_whole(coords, pieces):
    return pl.pallas_call(
        cotangent_kernel,
        out_shape=assembled_shapes(pieces),
        in_specs=[smem_spec()] + [vmem_spec()] * len(pieces),
        out_specs=(vmem_spec(), vmem_spec()),
        compiler_params=limits(12),
        name="cotangent_whole",
    )(coords, *pieces)


def normalized_whole(groups, coords, gain, pieces, tables):
    return pl.pallas_call(
        normalize_kernel,
        out_shape=assembled_shapes(pieces),
        in_specs=[smem_spec(), smem_spec()] + [vmem_spec()] * (1 + 2 * len(pieces)),
        out_specs=(vmem_spec(), vmem_spec()),
        compiler_params=limits(12),
        name="normalized_whole",
    )(in_hbm(groups), coords, gain, *pieces, *tables)


def rows_product(blocks, turned, right, outs, first):
    columns = slice(first, first + right.shape[1])
    half = len(blocks) // 2
    values = []
    for part in (blocks[:half], blocks[half:]):
        left = jnp.concatenate(
            [turned[pl.ds(pl.multiple_of(b * 128, 128), 128), :] for b in part], axis=0
        )
        values.append(jnp.dot(left, right, preferred_element_type=f32).astype(bf16))
    done = 0
    for out in outs:
        value, start = values[done // values[0].shape[0]], done % values[0].shape[0]
        out[:, columns] = value[start : start + out.shape[0], :]
        done += out.shape[0]


def hidden_kernel(p, lent):
    def kernel(coords, hid, hid_t, dy, dy_t, gate_w, up_w, down_w, hidden_t, ggi_t, gl_t, *outs):
        gate = jnp.dot(hid[...], gate_w[...], preferred_element_type=f32)
        lift = jnp.dot(hid[...], up_w[...], preferred_element_type=f32)
        grad = jnp.dot(dy[...], down_w[...], preferred_element_type=f32)
        sigma = jax.nn.sigmoid(gate)
        act = gate * sigma
        hidden = (act * lift).astype(bf16)
        ggi = (grad * lift * sigma * (1.0 + gate * (1.0 - sigma))).astype(bf16)
        gl = (grad * act).astype(bf16)
        own = row_blocks(coords, PATTERNS[p])
        rows_product(own, dy_t, hidden[:, lent:], outs[:3], 0)
        both = jnp.concatenate([ggi, gl], axis=1)
        rows_product(own, hid_t, both, outs[:3], hidden.shape[1] - lent)
        if lent:
            rows_product(row_blocks(coords, PATTERNS[0]), dy_t, hidden[:, :lent], outs[3:], 0)
        hidden_t[...] = hidden.T
        ggi_t[...] = ggi.T
        gl_t[...] = gl.T

    return kernel


def hidden_part(p, coords, hid, hid_t, dy, dy_t, gate_w, up_w, down_w):
    rows, width = hid.shape
    part = gate_w.shape[1] // RING
    lent = LENT if p == RING - 1 else 0

    def fixed(*shape):
        return pl.BlockSpec(shape, lambda i: (0, 0))

    weight = pl.BlockSpec((width, part), lambda i: (0, p))
    columns = 3 * part - lent
    shapes = [(part, rows)] * 3 + [(width // 4, columns)] * 2 + [(width // 2, columns)]
    shapes += [(width // 2, lent)] * 2 if lent else []
    return pl.pallas_call(
        hidden_kernel(p, lent),
        grid=(1,),
        out_shape=tuple(jax.ShapeDtypeStruct(shape, bf16) for shape in shapes),
        in_specs=[
            smem_spec(),
            fixed(rows, width),
            fixed(width, rows),
            fixed(rows, width),
            fixed(width, rows),
            weight,
            weight,
            weight,
        ],
        out_specs=tuple(fixed(*shape) for shape in shapes),
        compiler_params=limits(20),
        name="hidden_part",
    )(coords, hid, hid_t, dy, dy_t, gate_w, up_w, down_w)


def back_kernel(coords, *refs):
    acts, weights, outs = refs[: 3 * RING], refs[3 * RING : 3 * RING + 3], refs[3 * RING + 3 :]
    feat = outs[0].shape[1]
    whole = [
        jnp.concatenate([r[...] for r in acts[j * RING : (j + 1) * RING]], axis=0) for j in range(3)
    ]
    for other, out in ((1, outs[0]), (0, outs[1])):
        terms = []
        for weight, act in zip(weights, whole):
            left = jnp.concatenate(
                [
                    weight[pl.ds(pl.multiple_of(b * feat, feat), feat), :]
                    for b in feature_blocks(coords, other)
                ],
                axis=0,
            )
            terms.append(jnp.dot(left, act, preferred_element_type=f32))
        for j, total in enumerate((terms[0] + terms[1], terms[2])):
            for k in range(RING):
                out[j * RING + k] = total[k * feat : (k + 1) * feat, :].astype(bf16)


def back(coords, acts, weights):
    rows = acts[0][0].shape[1]
    feat = weights[0].shape[0] // (2 * RING)
    out = jax.ShapeDtypeStruct((2 * RING, feat, rows), bf16)
    return pl.pallas_call(
        back_kernel,
        in_specs=[smem_spec()] + [vmem_spec()] * (3 * RING + 3),
        out_specs=(vmem_spec(), vmem_spec()),
        out_shape=(out, out),
        compiler_params=limits(24),
        name="back",
    )(coords, *[a for group in acts for a in group], *weights)


def chip_sum_kernel(near, other, own, *sends):
    feat = near.shape[1]
    for j in range(2):
        rows = slice(j * feat, (j + 1) * feat)
        own[rows, :] = near[j * RING].astype(f32) + other[j * RING].astype(f32)
        for k, send in enumerate(sends, 1):
            i = j * RING + k
            send[rows, :] = (near[i].astype(f32) + other[i].astype(f32)).astype(bf16)


def mp_scattered(far, near):
    other = lax.ppermute(far, "c", CORES)
    piece = (2 * near.shape[1], near.shape[2])
    own, *sends = pl.pallas_call(
        chip_sum_kernel,
        out_shape=(jax.ShapeDtypeStruct(piece, f32),)
        + (jax.ShapeDtypeStruct(piece, bf16),) * (RING - 1),
        in_specs=[vmem_spec()] * 2,
        out_specs=(vmem_spec(),) * RING,
        compiler_params=limits(8),
        name="chip_sum",
    )(near, other)
    came = []
    for k in (1, 3, 2):
        came.append(lax.ppermute(sends[k - 1], "y", shift(k)))
    return own, came


def split_kernel(*refs):
    ins, (send, kept) = refs[:-2], refs[-2:]
    half = send.shape[0]
    first = 0
    for keep, came in zip(ins[::2], ins[1::2]):
        columns = slice(first, first + keep.shape[1])
        send[:, columns] = (keep[:half, :].astype(f32) + came[:half, :].astype(f32)).astype(bf16)
        kept[:, columns] = (keep[half:, :].astype(f32) + came[half:, :].astype(f32)).astype(bf16)
        first += keep.shape[1]


def split_add(*pairs):
    rows = pairs[0].shape[0] // 2
    half = jax.ShapeDtypeStruct((rows, sum(a.shape[1] for a in pairs[::2])), bf16)
    return pl.pallas_call(
        split_kernel,
        out_shape=(half, half),
        in_specs=[vmem_spec()] * len(pairs),
        out_specs=(vmem_spec(),) * 2,
        compiler_params=limits(8),
        name="split_add",
    )(*pairs)


def half_kernel(half, count):
    def kernel(*refs):
        ins, outs = refs[:-count], refs[-count:]
        rows = ins[0].shape[0] // 2
        first = 0
        for keep, came in zip(ins[::2], ins[1::2]):
            mine = keep[half * rows : (half + 1) * rows, :]
            start = half * rows if came.shape[0] > rows else 0
            theirs = came[start : start + rows, :]
            columns = slice(first, first + keep.shape[1])
            total = (mine.astype(f32) + theirs.astype(f32)).astype(bf16)
            for i, out in enumerate(outs):
                out[:, columns] = total[i * out.shape[0] : (i + 1) * out.shape[0], :]
            first += keep.shape[1]

    return kernel


def half_add(half, count, *pairs):
    rows = pairs[0].shape[0] // 2 // count
    out = jax.ShapeDtypeStruct((rows, sum(a.shape[1] for a in pairs[::2])), bf16)
    return pl.pallas_call(
        half_kernel(half, count),
        out_shape=(out,) * count,
        in_specs=[vmem_spec()] * len(pairs),
        out_specs=(vmem_spec(),) * count,
        compiler_params=limits(6),
        name="half_add",
    )(*pairs)


def sections(part):
    runs = []
    for p in range(RING):
        lent = LENT if p == RING - 1 else 0
        runs.append([(0, p * part + lent, part - lent), (1, p * part, part), (2, p * part, part)])
    runs[0].append((0, (RING - 1) * part, LENT))
    return runs


def finish_kernel(*refs):
    ins, outs = refs[: 2 * RING], refs[2 * RING :]
    for p, runs in enumerate(sections(outs[0].shape[1] // RING)):
        total = ins[2 * p][...].astype(f32) + ins[2 * p + 1][...].astype(f32)
        first = 0
        for out, column, width in runs:
            outs[out][:, column : column + width] = total[:, first : first + width]
            first += width


def finished(pairs, width):
    rows = pairs[0][0].shape[0]
    out = jax.ShapeDtypeStruct((rows, width), f32)
    return pl.pallas_call(
        finish_kernel,
        out_shape=(out,) * 3,
        in_specs=[vmem_spec()] * (2 * RING),
        out_specs=(vmem_spec(),) * 3,
        compiler_params=limits(6),
        name="finished",
    )(*[a for pair in pairs for a in pair])


def body(tokens, norm_gain, running_sq, gate_weight, up_weight, down_weight_t, groups, cotangent):
    tok_rows, feat = tokens.shape
    groups_total = tok_rows * RING * RING // GHOST
    coords = jnp.stack([lax.axis_index(a) for a in ("z", "x", "y", "c")]).astype(jnp.int32)
    gain = norm_gain.reshape(1, -1)
    local, both = stats(groups, coords, tokens, cotangent, groups_total)
    pieces = gathered(both)
    sums = ring_pieces(ring_sum(local, "z"), "x")
    table, quad = scale_table(sums)
    tables = gathered(table)
    (down_weight_t,) = staged(down_weight_t)
    gate_weight, up_weight = staged(gate_weight, up_weight)
    dy_full, dy_turned = cotangent_whole(coords, pieces)
    hid_full, hid_turned = normalized_whole(groups, coords, gain, pieces, tables)
    parts = []
    for p in range(RING):
        parts.append(
            hidden_part(
                p, coords, hid_full, hid_turned, dy_full, dy_turned, gate_weight, up_weight, down_weight_t
            )
        )
    last = []
    for p, (major, first) in enumerate(PATTERNS):
        minor = "x" if major == "z" else "z"
        pair = (NEAR, FAR) if first == 0 else (FAR, NEAR)
        send_a, send_b, keep = parts[p][3:6]
        more = ()
        if p == 0:
            more = (parts[-1][7], lax.ppermute(parts[-1][6], major, pair[0]))
        came_a = lax.ppermute(send_a, major, pair[0])
        came_b = lax.ppermute(send_b, major, pair[0])
        send_a, send_b = half_add(0, 2, keep, came_a, *more)
        next_a = lax.ppermute(send_a, major, pair[1])
        next_b = lax.ppermute(send_b, major, pair[1])
        (keep,) = half_add(1, 1, keep, came_b, *more)
        (send,) = half_add(0, 1, keep, next_a)
        came = lax.ppermute(send, minor, pair[0])
        (keep,) = half_add(1, 1, keep, next_b)
        send, keep = split_add(keep, came)
        came = lax.ppermute(send, minor, pair[1])
        last.append((keep, came))
    grad_down_t, grad_gate, grad_up = finished(last, gate_weight.shape[1])

    far, near = back(
        coords,
        [[q[1] for q in parts], [q[2] for q in parts], [q[0] for q in parts]],
        [gate_weight, up_weight, down_weight_t],
    )
    kept, came_y = mp_scattered(far, near)
    grad, local = partials(groups, tokens, table, kept, came_y)
    mine, came = tok_halves(local)
    grad_tokens, grad_gain = input_grads(groups, coords, tokens, cotangent, gain, table, grad, mine, came)

    block_out, running_new = branch_out(tokens, running_sq.reshape(1, feat), quad, kept, came_y)
    return (
        block_out,
        grad_tokens,
        running_new.reshape(feat),
        grad_gain.reshape(feat),
        grad_gate,
        grad_up,
        grad_down_t,
    )


def solution(mesh):
    torus = Mesh(mesh.devices.reshape(RING, RING, RING, 2), ("z", "x", "y", "c"))
    tok, mp = ("z", "x"), ("y", "c")
    placed = (P(tok, mp), P(), P(mp), P(None, mp), P(None, mp), P(None, mp), P(tok), P(tok, mp))
    out = (P(tok, mp), P(tok, mp), P(mp), P(mp), P(tok, mp), P(tok, mp), P(tok, mp))

    return jax.shard_map(body, mesh=torus, in_specs=placed, out_specs=out, check_vma=False)
```

```python
import jax
import jax.numpy as jnp
from jax import lax
from jax.experimental import pallas as pl
from jax.experimental.pallas import tpu as pltpu
from jax.sharding import Mesh
from jax.sharding import PartitionSpec as P


GHOST = 128
BLK = 16
RING = 4
NEAR = [(i, i ^ 1) for i in range(RING)]
FAR = [(i, RING - 1 - i) for i in range(RING)]
CORES = [(0, 1), (1, 0)]
EPSILON = 1e-05
MOMENTUM = 0.1


bf16 = jnp.bfloat16
f32 = jnp.float32


PATTERNS = (("z", 0), ("z", 1), ("x", 0), ("x", 1))
LENT = 128


def halving(i, first):
    near, far = i ^ 1, RING - 1 - i
    p, q = (near, far) if first == 0 else (far, near)
    return [RING - 1 - p if first == 0 else p ^ 1, p, q, i]


def row_blocks(coords, pattern):
    major, first = pattern
    hz, hx = halving(coords[0], first), halving(coords[1], first)
    if major == "z":
        return [RING * a + b for a in hz for b in hx]
    return [RING * a + b for b in hx for a in hz]


def feature_blocks(coords, other):
    core = coords[3] if other == 0 else 1 - coords[3]
    return [2 * ((coords[2] + k) & (RING - 1)) + core for k in range(RING)]


def shift(k):
    return [(i, (i + k) % RING) for i in range(RING)]


def vmem_spec():
    return pl.BlockSpec(memory_space=pltpu.VMEM)


def smem_spec():
    return pl.BlockSpec(memory_space=pltpu.SMEM)


def in_hbm(x):
    return pltpu.with_memory_space_constraint(x, pltpu.HBM)


def gathered(x):
    near = [x]
    for k in (1, 3, 2):
        near.append(lax.ppermute(x, "y", shift(-k)))
    near = [near[0], near[1], near[3], near[2]]
    far = []
    for k in range(RING):
        far.append(lax.ppermute(near[k], "c", CORES))
    return near + far


def block_sum(value):
    return jnp.sum(value, axis=0, keepdims=True)


def own_gain(coords, gain, feat):
    return gain[:, pl.ds(pl.multiple_of((2 * coords[2] + coords[3]) * feat, feat), feat)]


def add_kernel(left, right, out):
    out[...] = left[...] + right[...]


def pair_added(left, right):
    return pl.pallas_call(
        add_kernel,
        out_shape=jax.ShapeDtypeStruct(left.shape, left.dtype),
        in_specs=[vmem_spec()] * 2,
        out_specs=vmem_spec(),
        compiler_params=limits(1),
        name="pair_added",
    )(left, right)


def tok_halves(x):
    for i, (axis, pairs) in enumerate((("z", NEAR), ("z", FAR), ("x", NEAR), ("x", FAR)), 1):
        came = lax.ppermute(x, axis, pairs)
        if i < 4:
            x = pair_added(x, came)
    return x, came


def ring_sum_kernel(*refs):
    ins, out = refs[:-1], refs[-1]
    out[...] = (ins[0][...] + ins[3][...]) + (ins[1][...] + ins[2][...])


def ring_pieces(x, axis):
    came = [x]
    for k in (1, 3, 2):
        came.append(lax.ppermute(x, axis, shift(k)))
    return came


def ring_sum(x, axis):
    pieces = ring_pieces(x, axis)
    return pl.pallas_call(
        ring_sum_kernel,
        out_shape=jax.ShapeDtypeStruct(x.shape, x.dtype),
        in_specs=[vmem_spec()] * RING,
        out_specs=vmem_spec(),
        compiler_params=limits(1),
        name="ring_sum",
    )(*pieces)


STAGE_CUTS = 4


def stage_kernel(*refs):
    count = (len(refs) - 1) // 2
    sems = refs[-1]
    copies = []
    for i in range(count):
        source, out = refs[i], refs[count + i]
        rows = source.shape[0] // STAGE_CUTS
        for j in range(STAGE_CUTS):
            part = pl.ds(j * rows, rows)
            copies.append(
                pltpu.make_async_copy(source.at[part], out.at[part], sems.at[i * STAGE_CUTS + j])
            )
    for copy in copies:
        copy.start()
    for copy in copies:
        copy.wait()


def staged(*weights):
    return pl.pallas_call(
        stage_kernel,
        out_shape=tuple(pltpu.VMEM(w.shape, w.dtype) for w in weights),
        in_specs=[pl.BlockSpec(memory_space=pltpu.HBM)] * len(weights),
        out_specs=(vmem_spec(),) * len(weights),
        scratch_shapes=[pltpu.SemaphoreType.DMA((STAGE_CUTS * len(weights),))],
        compiler_params=limits(1),
        name="staged",
    )(*[in_hbm(w) for w in weights])


def stats_kernel(groups, coords, tokens, cotangent, out, both):
    rows = tokens.shape[0]
    both[:rows, :] = tokens[...]
    both[rows:, :] = cotangent[...]
    out[...] = jnp.zeros_like(out)
    for b in range(rows // BLK):
        value = tokens[b * BLK : (b + 1) * BLK, :].astype(f32)
        row = pl.ds(groups[b], 1)
        out[row, :] = out[row, :] + block_sum(value * value)


def stats(groups, coords, tokens, cotangent, groups_total):
    rows, feat = tokens.shape
    return pl.pallas_call(
        stats_kernel,
        out_shape=(
            jax.ShapeDtypeStruct((groups_total, feat), f32),
            jax.ShapeDtypeStruct((2 * rows, feat), bf16),
        ),
        in_specs=[smem_spec(), smem_spec(), vmem_spec(), vmem_spec()],
        out_specs=(vmem_spec(),) * 2,
        compiler_params=limits(4),
        name="stats",
    )(in_hbm(groups), coords, in_hbm(tokens), in_hbm(cotangent))


def table_kernel(a, b, c, d, table, quad):
    quad_mean = ((a[...] + d[...]) + (b[...] + c[...])) * (1.0 / GHOST)
    quad[...] = quad_mean
    table[...] = lax.rsqrt(quad_mean + EPSILON)


def scale_table(pieces):
    out = jax.ShapeDtypeStruct(pieces[0].shape, f32)
    return pl.pallas_call(
        table_kernel,
        out_shape=(out, out),
        in_specs=[vmem_spec()] * RING,
        out_specs=(vmem_spec(),) * 2,
        compiler_params=limits(2),
        name="scale_table",
    )(*pieces)


def partial_kernel(groups, tokens, table, own, *refs):
    came, (grad, out) = refs[:-2], refs[-2:]
    feat = tokens.shape[1]
    total = own[:feat, :]
    for ref in came:
        total = total + ref[:feat, :].astype(f32)
    grad[...] = total.T
    out[...] = jnp.zeros_like(out)
    for b in range(tokens.shape[0] // BLK):
        rows = slice(b * BLK, (b + 1) * BLK)
        row = pl.ds(groups[b], 1)
        normed = tokens[rows, :].astype(f32) * table[row, :]
        out[row, :] = out[row, :] + block_sum(grad[rows, :] * normed)


def partials(groups, tokens, table, own, came):
    rows, feat = tokens.shape
    return pl.pallas_call(
        partial_kernel,
        out_shape=(
            jax.ShapeDtypeStruct((rows, feat), f32),
            jax.ShapeDtypeStruct(table.shape, f32),
        ),
        in_specs=[smem_spec()] + [vmem_spec()] * (3 + len(came)),
        out_specs=(vmem_spec(),) * 2,
        compiler_params=limits(6),
        name="partials",
    )(in_hbm(groups), tokens, table, own, *came)


def input_kernel(groups, coords, tokens, cotangent, gain, table, grad, mine, came, out, grad_gain, acc):
    partial = mine[...] + came[...]
    grad_gain[...] = jnp.sum(partial, axis=0, keepdims=True)
    gain_row = own_gain(coords, gain, tokens.shape[1])
    acc[...] = gain_row * partial * (1.0 / GHOST)
    for b in range(tokens.shape[0] // BLK):
        rows = slice(b * BLK, (b + 1) * BLK)
        row = pl.ds(groups[b], 1)
        scale = table[row, :]
        normed = tokens[rows, :].astype(f32) * scale
        inner = gain_row * grad[rows, :] - normed * acc[row, :]
        out[rows, :] = (cotangent[rows, :].astype(f32) + scale * inner).astype(bf16)


def input_grads(groups, coords, tokens, cotangent, gain, table, grad, mine, came):
    rows, feat = tokens.shape
    return pl.pallas_call(
        input_kernel,
        out_shape=(
            jax.ShapeDtypeStruct((rows, feat), bf16),
            jax.ShapeDtypeStruct((1, feat), f32),
        ),
        in_specs=[smem_spec(), smem_spec()] + [vmem_spec()] * 7,
        out_specs=(vmem_spec(),) * 2,
        scratch_shapes=[pltpu.VMEM(table.shape, f32)],
        compiler_params=limits(6),
        name="input_grads",
    )(in_hbm(groups), coords, tokens, cotangent, gain, table, grad, mine, came)


def branch_kernel(tokens, running, quad, own, *refs):
    came, (out, running_new) = refs[:-2], refs[-2:]
    feat = tokens.shape[1]
    total = own[feat:, :]
    for ref in came:
        total = total + ref[feat:, :].astype(f32)
    out[...] = (tokens[...].astype(f32) + total.T).astype(bf16)
    mean = jnp.sum(quad[...], axis=0, keepdims=True) / quad.shape[0]
    running_new[...] = (1.0 - MOMENTUM) * running[...] + MOMENTUM * mean


def branch_out(tokens, running, quad, own, came):
    return pl.pallas_call(
        branch_kernel,
        out_shape=(
            jax.ShapeDtypeStruct(tokens.shape, bf16),
            jax.ShapeDtypeStruct(running.shape, f32),
        ),
        in_specs=[vmem_spec()] * (4 + len(came)),
        out_specs=(vmem_spec(),) * 2,
        compiler_params=limits(6),
        name="branch_out",
    )(tokens, in_hbm(running), quad, own, *came)


def limits(mib):
    return pltpu.CompilerParams(vmem_limit_bytes=mib << 20)


def places(coords):
    return feature_blocks(coords, 0) + feature_blocks(coords, 1)


def cotangent_kernel(coords, *refs):
    pieces, (out, turned) = refs[:-2], refs[-2:]
    rows, width = out.shape[0], pieces[0].shape[1]
    for place, piece in zip(places(coords), pieces):
        first = pl.multiple_of(place * width, width)
        value = piece[rows:, :]
        out[:, pl.ds(first, width)] = value
        turned[pl.ds(first, width), :] = value.T


def normalize_kernel(groups, coords, gain, *refs):
    ins, (out, turned) = refs[:-2], refs[-2:]
    pieces, tables = ins[: len(ins) // 2], ins[len(ins) // 2 :]
    rows, width = out.shape[0], pieces[0].shape[1]
    for place, piece, table in zip(places(coords), pieces, tables):
        first = pl.multiple_of(place * width, width)
        gain_row = gain[:, pl.ds(first, width)]
        for b in range(rows // BLK):
            block = slice(b * BLK, (b + 1) * BLK)
            normed = piece[block, :].astype(f32) * table[pl.ds(groups[b], 1), :]
            out[block, pl.ds(first, width)] = (gain_row * normed).astype(bf16)
        turned[pl.ds(first, width), :] = out[:, pl.ds(first, width)].T


def assembled_shapes(pieces):
    rows, width = pieces[0].shape[0] // 2, pieces[0].shape[1] * len(pieces)
    return (jax.ShapeDtypeStruct((rows, width), bf16), jax.ShapeDtypeStruct((width, rows), bf16))


def cotangent_whole(coords, pieces):
    return pl.pallas_call(
        cotangent_kernel,
        out_shape=assembled_shapes(pieces),
        in_specs=[smem_spec()] + [vmem_spec()] * len(pieces),
        out_specs=(vmem_spec(), vmem_spec()),
        compiler_params=limits(12),
        name="cotangent_whole",
    )(coords, *pieces)


def normalized_whole(groups, coords, gain, pieces, tables):
    return pl.pallas_call(
        normalize_kernel,
        out_shape=assembled_shapes(pieces),
        in_specs=[smem_spec(), smem_spec()] + [vmem_spec()] * (1 + 2 * len(pieces)),
        out_specs=(vmem_spec(), vmem_spec()),
        compiler_params=limits(12),
        name="normalized_whole",
    )(in_hbm(groups), coords, gain, *pieces, *tables)


def rows_product(blocks, turned, right, outs, first):
    columns = slice(first, first + right.shape[1])
    half = len(blocks) // 2
    values = []
    for part in (blocks[:half], blocks[half:]):
        left = jnp.concatenate(
            [turned[pl.ds(pl.multiple_of(b * 128, 128), 128), :] for b in part], axis=0
        )
        values.append(jnp.dot(left, right, preferred_element_type=f32).astype(bf16))
    done = 0
    for out in outs:
        value, start = values[done // values[0].shape[0]], done % values[0].shape[0]
        out[:, columns] = value[start : start + out.shape[0], :]
        done += out.shape[0]


def hidden_kernel(p, lent):
    def kernel(coords, hid, hid_t, dy, dy_t, gate_w, up_w, down_w, hidden_t, ggi_t, gl_t, *outs):
        gate = jnp.dot(hid[...], gate_w[...], preferred_element_type=f32)
        lift = jnp.dot(hid[...], up_w[...], preferred_element_type=f32)
        grad = jnp.dot(dy[...], down_w[...], preferred_element_type=f32)
        sigma = jax.nn.sigmoid(gate)
        act = gate * sigma
        hidden = (act * lift).astype(bf16)
        ggi = (grad * lift * sigma * (1.0 + gate * (1.0 - sigma))).astype(bf16)
        gl = (grad * act).astype(bf16)
        own = row_blocks(coords, PATTERNS[p])
        rows_product(own, dy_t, hidden[:, lent:], outs[:3], 0)
        both = jnp.concatenate([ggi, gl], axis=1)
        rows_product(own, hid_t, both, outs[:3], hidden.shape[1] - lent)
        if lent:
            rows_product(row_blocks(coords, PATTERNS[0]), dy_t, hidden[:, :lent], outs[3:], 0)
        hidden_t[...] = hidden.T
        ggi_t[...] = ggi.T
        gl_t[...] = gl.T

    return kernel


def hidden_part(p, coords, hid, hid_t, dy, dy_t, gate_w, up_w, down_w):
    rows, width = hid.shape
    part = gate_w.shape[1] // RING
    lent = LENT if p == RING - 1 else 0

    def fixed(*shape):
        return pl.BlockSpec(shape, lambda i: (0, 0))

    weight = pl.BlockSpec((width, part), lambda i: (0, p))
    columns = 3 * part - lent
    shapes = [(part, rows)] * 3 + [(width // 4, columns)] * 2 + [(width // 2, columns)]
    shapes += [(width // 2, lent)] * 2 if lent else []
    return pl.pallas_call(
        hidden_kernel(p, lent),
        grid=(1,),
        out_shape=tuple(jax.ShapeDtypeStruct(shape, bf16) for shape in shapes),
        in_specs=[
            smem_spec(),
            fixed(rows, width),
            fixed(width, rows),
            fixed(rows, width),
            fixed(width, rows),
            weight,
            weight,
            weight,
        ],
        out_specs=tuple(fixed(*shape) for shape in shapes),
        compiler_params=limits(20),
        name="hidden_part",
    )(coords, hid, hid_t, dy, dy_t, gate_w, up_w, down_w)


def back_kernel(coords, *refs):
    acts, weights = refs[: 3 * RING], refs[3 * RING : 3 * RING + 3]
    outs, whole = refs[3 * RING + 3 : -1], refs[-1]
    feat, part = outs[0].shape[1], acts[0].shape[0]
    for j in range(3):
        for p in range(RING):
            whole[j, p * part : (p + 1) * part, :] = acts[j * RING + p][...]
    for other, out in ((1, outs[0]), (0, outs[1])):
        core = coords[3] if other == 0 else 1 - coords[3]

        def step(k, carry, core=core, out=out):
            block = 2 * ((coords[2] + k) & (RING - 1)) + core
            rows = pl.ds(pl.multiple_of(block * feat, feat), feat)
            terms = [
                jnp.dot(weight[rows, :], whole[j], preferred_element_type=f32)
                for j, weight in enumerate(weights)
            ]
            out[k] = (terms[0] + terms[1]).astype(bf16)
            out[RING + k] = terms[2].astype(bf16)
            return carry

        lax.fori_loop(0, RING, step, 0)


def back(coords, acts, weights):
    rows = acts[0][0].shape[1]
    feat = weights[0].shape[0] // (2 * RING)
    out = jax.ShapeDtypeStruct((2 * RING, feat, rows), bf16)
    return pl.pallas_call(
        back_kernel,
        in_specs=[smem_spec()] + [vmem_spec()] * (3 * RING + 3),
        out_specs=(vmem_spec(), vmem_spec()),
        out_shape=(out, out),
        scratch_shapes=[pltpu.VMEM((3, weights[0].shape[1], rows), bf16)],
        compiler_params=limits(20),
        name="back",
    )(coords, *[a for group in acts for a in group], *weights)


def chip_sum_kernel(near, other, own, *sends):
    feat = near.shape[1]
    for j in range(2):
        rows = slice(j * feat, (j + 1) * feat)
        own[rows, :] = near[j * RING].astype(f32) + other[j * RING].astype(f32)
        for k, send in enumerate(sends, 1):
            i = j * RING + k
            send[rows, :] = (near[i].astype(f32) + other[i].astype(f32)).astype(bf16)


def mp_scattered(far, near):
    other = lax.ppermute(far, "c", CORES)
    piece = (2 * near.shape[1], near.shape[2])
    own, *sends = pl.pallas_call(
        chip_sum_kernel,
        out_shape=(jax.ShapeDtypeStruct(piece, f32),)
        + (jax.ShapeDtypeStruct(piece, bf16),) * (RING - 1),
        in_specs=[vmem_spec()] * 2,
        out_specs=(vmem_spec(),) * RING,
        compiler_params=limits(8),
        name="chip_sum",
    )(near, other)
    came = []
    for k in (1, 3, 2):
        came.append(lax.ppermute(sends[k - 1], "y", shift(k)))
    return own, came


def split_kernel(*refs):
    ins, (send, kept) = refs[:-2], refs[-2:]
    half = send.shape[0]
    first = 0
    for keep, came in zip(ins[::2], ins[1::2]):
        columns = slice(first, first + keep.shape[1])
        send[:, columns] = (keep[:half, :].astype(f32) + came[:half, :].astype(f32)).astype(bf16)
        kept[:, columns] = (keep[half:, :].astype(f32) + came[half:, :].astype(f32)).astype(bf16)
        first += keep.shape[1]


def split_add(*pairs):
    rows = pairs[0].shape[0] // 2
    half = jax.ShapeDtypeStruct((rows, sum(a.shape[1] for a in pairs[::2])), bf16)
    return pl.pallas_call(
        split_kernel,
        out_shape=(half, half),
        in_specs=[vmem_spec()] * len(pairs),
        out_specs=(vmem_spec(),) * 2,
        compiler_params=limits(8),
        name="split_add",
    )(*pairs)


def half_kernel(half, count):
    def kernel(*refs):
        ins, outs = refs[:-count], refs[-count:]
        rows = ins[0].shape[0] // 2
        first = 0
        for keep, came in zip(ins[::2], ins[1::2]):
            mine = keep[half * rows : (half + 1) * rows, :]
            start = half * rows if came.shape[0] > rows else 0
            theirs = came[start : start + rows, :]
            columns = slice(first, first + keep.shape[1])
            total = (mine.astype(f32) + theirs.astype(f32)).astype(bf16)
            for i, out in enumerate(outs):
                out[:, columns] = total[i * out.shape[0] : (i + 1) * out.shape[0], :]
            first += keep.shape[1]

    return kernel


def half_add(half, count, *pairs):
    rows = pairs[0].shape[0] // 2 // count
    out = jax.ShapeDtypeStruct((rows, sum(a.shape[1] for a in pairs[::2])), bf16)
    return pl.pallas_call(
        half_kernel(half, count),
        out_shape=(out,) * count,
        in_specs=[vmem_spec()] * len(pairs),
        out_specs=(vmem_spec(),) * count,
        compiler_params=limits(6),
        name="half_add",
    )(*pairs)


def sections(part):
    runs = []
    for p in range(RING):
        lent = LENT if p == RING - 1 else 0
        runs.append([(0, p * part + lent, part - lent), (1, p * part, part), (2, p * part, part)])
    runs[0].append((0, (RING - 1) * part, LENT))
    return runs


def finish_kernel(*refs):
    ins, outs = refs[: 2 * RING], refs[2 * RING :]
    for p, runs in enumerate(sections(outs[0].shape[1] // RING)):
        total = ins[2 * p][...].astype(f32) + ins[2 * p + 1][...].astype(f32)
        first = 0
        for out, column, width in runs:
            outs[out][:, column : column + width] = total[:, first : first + width]
            first += width


def finished(pairs, width):
    rows = pairs[0][0].shape[0]
    out = jax.ShapeDtypeStruct((rows, width), f32)
    return pl.pallas_call(
        finish_kernel,
        out_shape=(out,) * 3,
        in_specs=[vmem_spec()] * (2 * RING),
        out_specs=(vmem_spec(),) * 3,
        compiler_params=limits(6),
        name="finished",
    )(*[a for pair in pairs for a in pair])


def body(tokens, norm_gain, running_sq, gate_weight, up_weight, down_weight_t, groups, cotangent):
    tok_rows, feat = tokens.shape
    groups_total = tok_rows * RING * RING // GHOST
    coords = jnp.stack([lax.axis_index(a) for a in ("z", "x", "y", "c")]).astype(jnp.int32)
    gain = norm_gain.reshape(1, -1)
    local, both = stats(groups, coords, tokens, cotangent, groups_total)
    pieces = gathered(both)
    sums = ring_pieces(ring_sum(local, "z"), "x")
    table, quad = scale_table(sums)
    tables = gathered(table)
    (down_weight_t,) = staged(down_weight_t)
    gate_weight, up_weight = staged(gate_weight, up_weight)
    dy_full, dy_turned = cotangent_whole(coords, pieces)
    hid_full, hid_turned = normalized_whole(groups, coords, gain, pieces, tables)
    parts = []
    for p in range(RING):
        parts.append(
            hidden_part(
                p, coords, hid_full, hid_turned, dy_full, dy_turned, gate_weight, up_weight, down_weight_t
            )
        )
    last = []
    for p, (major, first) in enumerate(PATTERNS):
        minor = "x" if major == "z" else "z"
        pair = (NEAR, FAR) if first == 0 else (FAR, NEAR)
        send_a, send_b, keep = parts[p][3:6]
        more = ()
        if p == 0:
            more = (parts[-1][7], lax.ppermute(parts[-1][6], major, pair[0]))
        came_a = lax.ppermute(send_a, major, pair[0])
        came_b = lax.ppermute(send_b, major, pair[0])
        send_a, send_b = half_add(0, 2, keep, came_a, *more)
        next_a = lax.ppermute(send_a, major, pair[1])
        next_b = lax.ppermute(send_b, major, pair[1])
        (keep,) = half_add(1, 1, keep, came_b, *more)
        (send,) = half_add(0, 1, keep, next_a)
        came = lax.ppermute(send, minor, pair[0])
        (keep,) = half_add(1, 1, keep, next_b)
        send, keep = split_add(keep, came)
        came = lax.ppermute(send, minor, pair[1])
        last.append((keep, came))
    grad_down_t, grad_gate, grad_up = finished(last, gate_weight.shape[1])

    far, near = back(
        coords,
        [[q[1] for q in parts], [q[2] for q in parts], [q[0] for q in parts]],
        [gate_weight, up_weight, down_weight_t],
    )
    kept, came_y = mp_scattered(far, near)
    grad, local = partials(groups, tokens, table, kept, came_y)
    mine, came = tok_halves(local)
    grad_tokens, grad_gain = input_grads(groups, coords, tokens, cotangent, gain, table, grad, mine, came)

    block_out, running_new = branch_out(tokens, running_sq.reshape(1, feat), quad, kept, came_y)
    return (
        block_out,
        grad_tokens,
        running_new.reshape(feat),
        grad_gain.reshape(feat),
        grad_gate,
        grad_up,
        grad_down_t,
    )


def solution(mesh):
    torus = Mesh(mesh.devices.reshape(RING, RING, RING, 2), ("z", "x", "y", "c"))
    tok, mp = ("z", "x"), ("y", "c")
    placed = (P(tok, mp), P(), P(mp), P(None, mp), P(None, mp), P(None, mp), P(tok), P(tok, mp))
    out = (P(tok, mp), P(tok, mp), P(mp), P(mp), P(tok, mp), P(tok, mp), P(tok, mp))

    return jax.shard_map(body, mesh=torus, in_specs=placed, out_specs=out, check_vma=False)
```

```python
import jax
import jax.numpy as jnp
from jax import lax
from jax.experimental import pallas as pl
from jax.experimental.pallas import tpu as pltpu
from jax.sharding import Mesh
from jax.sharding import PartitionSpec as P


GHOST = 128
BLK = 16
RING = 4
NEAR = [(i, i ^ 1) for i in range(RING)]
FAR = [(i, RING - 1 - i) for i in range(RING)]
CORES = [(0, 1), (1, 0)]
EPSILON = 1e-05
MOMENTUM = 0.1


bf16 = jnp.bfloat16
f32 = jnp.float32


PATTERNS = (("z", 0), ("z", 1), ("x", 0), ("x", 1))
LENT = 128


def halving(i, first):
    near, far = i ^ 1, RING - 1 - i
    p, q = (near, far) if first == 0 else (far, near)
    return [RING - 1 - p if first == 0 else p ^ 1, p, q, i]


def row_blocks(coords, pattern):
    major, first = pattern
    hz, hx = halving(coords[0], first), halving(coords[1], first)
    if major == "z":
        return [RING * a + b for a in hz for b in hx]
    return [RING * a + b for b in hx for a in hz]


def feature_blocks(coords, other):
    core = coords[3] if other == 0 else 1 - coords[3]
    return [2 * ((coords[2] + k) & (RING - 1)) + core for k in range(RING)]


def shift(k):
    return [(i, (i + k) % RING) for i in range(RING)]


def vmem_spec():
    return pl.BlockSpec(memory_space=pltpu.VMEM)


def smem_spec():
    return pl.BlockSpec(memory_space=pltpu.SMEM)


def in_hbm(x):
    return pltpu.with_memory_space_constraint(x, pltpu.HBM)


def gathered(x):
    near = [x]
    for k in (1, 3, 2):
        near.append(lax.ppermute(x, "y", shift(-k)))
    near = [near[0], near[1], near[3], near[2]]
    far = []
    for k in range(RING):
        far.append(lax.ppermute(near[k], "c", CORES))
    return near + far


def block_sum(value):
    return jnp.sum(value, axis=0, keepdims=True)


def own_gain(coords, gain, feat):
    return gain[:, pl.ds(pl.multiple_of((2 * coords[2] + coords[3]) * feat, feat), feat)]


def add_kernel(left, right, out):
    out[...] = left[...] + right[...]


def pair_added(left, right):
    return pl.pallas_call(
        add_kernel,
        out_shape=jax.ShapeDtypeStruct(left.shape, left.dtype),
        in_specs=[vmem_spec()] * 2,
        out_specs=vmem_spec(),
        compiler_params=limits(1),
        name="pair_added",
    )(left, right)


def tok_halves(x):
    for i, (axis, pairs) in enumerate((("z", NEAR), ("z", FAR), ("x", NEAR), ("x", FAR)), 1):
        came = lax.ppermute(x, axis, pairs)
        if i < 4:
            x = pair_added(x, came)
    return x, came


def ring_sum_kernel(*refs):
    ins, out = refs[:-1], refs[-1]
    out[...] = (ins[0][...] + ins[3][...]) + (ins[1][...] + ins[2][...])


def ring_pieces(x, axis):
    came = [x]
    for k in (1, 3, 2):
        came.append(lax.ppermute(x, axis, shift(k)))
    return came


def ring_sum(x, axis):
    pieces = ring_pieces(x, axis)
    return pl.pallas_call(
        ring_sum_kernel,
        out_shape=jax.ShapeDtypeStruct(x.shape, x.dtype),
        in_specs=[vmem_spec()] * RING,
        out_specs=vmem_spec(),
        compiler_params=limits(1),
        name="ring_sum",
    )(*pieces)


STAGE_CUTS = 4


def stage_kernel(*refs):
    count = (len(refs) - 1) // 2
    sems = refs[-1]
    copies = []
    for i in range(count):
        source, out = refs[i], refs[count + i]
        rows = source.shape[0] // STAGE_CUTS
        for j in range(STAGE_CUTS):
            part = pl.ds(j * rows, rows)
            copies.append(
                pltpu.make_async_copy(source.at[part], out.at[part], sems.at[i * STAGE_CUTS + j])
            )
    for copy in copies:
        copy.start()
    for copy in copies:
        copy.wait()


def staged(*weights):
    return pl.pallas_call(
        stage_kernel,
        out_shape=tuple(pltpu.VMEM(w.shape, w.dtype) for w in weights),
        in_specs=[pl.BlockSpec(memory_space=pltpu.HBM)] * len(weights),
        out_specs=(vmem_spec(),) * len(weights),
        scratch_shapes=[pltpu.SemaphoreType.DMA((STAGE_CUTS * len(weights),))],
        compiler_params=limits(1),
        name="staged",
    )(*[in_hbm(w) for w in weights])


def stats_kernel(groups, coords, tokens, cotangent, out, both):
    rows = tokens.shape[0]
    both[:rows, :] = tokens[...]
    both[rows:, :] = cotangent[...]
    out[...] = jnp.zeros_like(out)
    for b in range(rows // BLK):
        value = tokens[b * BLK : (b + 1) * BLK, :].astype(f32)
        row = pl.ds(groups[b], 1)
        out[row, :] = out[row, :] + block_sum(value * value)


def stats(groups, coords, tokens, cotangent, groups_total):
    rows, feat = tokens.shape
    return pl.pallas_call(
        stats_kernel,
        out_shape=(
            jax.ShapeDtypeStruct((groups_total, feat), f32),
            jax.ShapeDtypeStruct((2 * rows, feat), bf16),
        ),
        in_specs=[smem_spec(), smem_spec(), vmem_spec(), vmem_spec()],
        out_specs=(vmem_spec(),) * 2,
        compiler_params=limits(4),
        name="stats",
    )(in_hbm(groups), coords, in_hbm(tokens), in_hbm(cotangent))


def table_kernel(a, b, c, d, table, quad):
    quad_mean = ((a[...] + d[...]) + (b[...] + c[...])) * (1.0 / GHOST)
    quad[...] = quad_mean
    table[...] = lax.rsqrt(quad_mean + EPSILON)


def scale_table(pieces):
    out = jax.ShapeDtypeStruct(pieces[0].shape, f32)
    return pl.pallas_call(
        table_kernel,
        out_shape=(out, out),
        in_specs=[vmem_spec()] * RING,
        out_specs=(vmem_spec(),) * 2,
        compiler_params=limits(2),
        name="scale_table",
    )(*pieces)


def partial_kernel(groups, tokens, table, own, *refs):
    came, (grad, out) = refs[:-2], refs[-2:]
    feat = tokens.shape[1]
    total = own[:feat, :]
    for ref in came:
        total = total + ref[:feat, :].astype(f32)
    grad[...] = total.T
    out[...] = jnp.zeros_like(out)
    for b in range(tokens.shape[0] // BLK):
        rows = slice(b * BLK, (b + 1) * BLK)
        row = pl.ds(groups[b], 1)
        normed = tokens[rows, :].astype(f32) * table[row, :]
        out[row, :] = out[row, :] + block_sum(grad[rows, :] * normed)


def partials(groups, tokens, table, own, came):
    rows, feat = tokens.shape
    return pl.pallas_call(
        partial_kernel,
        out_shape=(
            jax.ShapeDtypeStruct((rows, feat), f32),
            jax.ShapeDtypeStruct(table.shape, f32),
        ),
        in_specs=[smem_spec()] + [vmem_spec()] * (3 + len(came)),
        out_specs=(vmem_spec(),) * 2,
        compiler_params=limits(6),
        name="partials",
    )(in_hbm(groups), tokens, table, own, *came)


def input_kernel(groups, coords, tokens, cotangent, gain, table, grad, mine, came, out, grad_gain, acc):
    partial = mine[...] + came[...]
    grad_gain[...] = jnp.sum(partial, axis=0, keepdims=True)
    gain_row = own_gain(coords, gain, tokens.shape[1])
    acc[...] = gain_row * partial * (1.0 / GHOST)
    for b in range(tokens.shape[0] // BLK):
        rows = slice(b * BLK, (b + 1) * BLK)
        row = pl.ds(groups[b], 1)
        scale = table[row, :]
        normed = tokens[rows, :].astype(f32) * scale
        inner = gain_row * grad[rows, :] - normed * acc[row, :]
        out[rows, :] = (cotangent[rows, :].astype(f32) + scale * inner).astype(bf16)


def branch_kernel(tokens, running, quad, own, *refs):
    came, (out, running_new) = refs[:-2], refs[-2:]
    feat = tokens.shape[1]
    total = own[feat:, :]
    for ref in came:
        total = total + ref[feat:, :].astype(f32)
    out[...] = (tokens[...].astype(f32) + total.T).astype(bf16)
    mean = jnp.sum(quad[...], axis=0, keepdims=True) / quad.shape[0]
    running_new[...] = (1.0 - MOMENTUM) * running[...] + MOMENTUM * mean


def branch_out(tokens, running, quad, own, came):
    return pl.pallas_call(
        branch_kernel,
        out_shape=(
            jax.ShapeDtypeStruct(tokens.shape, bf16),
            jax.ShapeDtypeStruct(running.shape, f32),
        ),
        in_specs=[vmem_spec()] * (4 + len(came)),
        out_specs=(vmem_spec(),) * 2,
        compiler_params=limits(6),
        name="branch_out",
    )(tokens, in_hbm(running), quad, own, *came)


def limits(mib):
    return pltpu.CompilerParams(vmem_limit_bytes=mib << 20)


def places(coords):
    return feature_blocks(coords, 0) + feature_blocks(coords, 1)


def cotangent_kernel(coords, *refs):
    pieces, (out, turned) = refs[:-2], refs[-2:]
    rows, width = out.shape[0], pieces[0].shape[1]
    for place, piece in zip(places(coords), pieces):
        first = pl.multiple_of(place * width, width)
        value = piece[rows:, :]
        out[:, pl.ds(first, width)] = value
        turned[pl.ds(first, width), :] = value.T


def normalize_kernel(groups, coords, gain, *refs):
    ins, (out, turned) = refs[:-2], refs[-2:]
    pieces, tables = ins[: len(ins) // 2], ins[len(ins) // 2 :]
    rows, width = out.shape[0], pieces[0].shape[1]
    for place, piece, table in zip(places(coords), pieces, tables):
        first = pl.multiple_of(place * width, width)
        gain_row = gain[:, pl.ds(first, width)]
        for b in range(rows // BLK):
            block = slice(b * BLK, (b + 1) * BLK)
            normed = piece[block, :].astype(f32) * table[pl.ds(groups[b], 1), :]
            out[block, pl.ds(first, width)] = (gain_row * normed).astype(bf16)
        turned[pl.ds(first, width), :] = out[:, pl.ds(first, width)].T


def assembled_shapes(pieces):
    rows, width = pieces[0].shape[0] // 2, pieces[0].shape[1] * len(pieces)
    return (jax.ShapeDtypeStruct((rows, width), bf16), jax.ShapeDtypeStruct((width, rows), bf16))


def cotangent_whole(coords, pieces):
    return pl.pallas_call(
        cotangent_kernel,
        out_shape=assembled_shapes(pieces),
        in_specs=[smem_spec()] + [vmem_spec()] * len(pieces),
        out_specs=(vmem_spec(), vmem_spec()),
        compiler_params=limits(12),
        name="cotangent_whole",
    )(coords, *pieces)


def normalized_whole(groups, coords, gain, pieces, tables):
    return pl.pallas_call(
        normalize_kernel,
        out_shape=assembled_shapes(pieces),
        in_specs=[smem_spec(), smem_spec()] + [vmem_spec()] * (1 + 2 * len(pieces)),
        out_specs=(vmem_spec(), vmem_spec()),
        compiler_params=limits(12),
        name="normalized_whole",
    )(in_hbm(groups), coords, gain, *pieces, *tables)


def rows_product(blocks, turned, right, outs, first):
    columns = slice(first, first + right.shape[1])
    half = len(blocks) // 2
    values = []
    for part in (blocks[:half], blocks[half:]):
        left = jnp.concatenate(
            [turned[pl.ds(pl.multiple_of(b * 128, 128), 128), :] for b in part], axis=0
        )
        values.append(jnp.dot(left, right, preferred_element_type=f32).astype(bf16))
    done = 0
    for out in outs:
        value, start = values[done // values[0].shape[0]], done % values[0].shape[0]
        out[:, columns] = value[start : start + out.shape[0], :]
        done += out.shape[0]


def hidden_kernel(p, lent):
    def kernel(coords, hid, hid_t, dy, dy_t, gate_w, up_w, down_w, hidden_t, ggi_t, gl_t, *outs):
        gate = jnp.dot(hid[...], gate_w[...], preferred_element_type=f32)
        lift = jnp.dot(hid[...], up_w[...], preferred_element_type=f32)
        grad = jnp.dot(dy[...], down_w[...], preferred_element_type=f32)
        sigma = jax.nn.sigmoid(gate)
        act = gate * sigma
        hidden = (act * lift).astype(bf16)
        ggi = (grad * lift * sigma * (1.0 + gate * (1.0 - sigma))).astype(bf16)
        gl = (grad * act).astype(bf16)
        own = row_blocks(coords, PATTERNS[p])
        rows_product(own, dy_t, hidden[:, lent:], outs[:3], 0)
        both = jnp.concatenate([ggi, gl], axis=1)
        rows_product(own, hid_t, both, outs[:3], hidden.shape[1] - lent)
        if lent:
            rows_product(row_blocks(coords, PATTERNS[0]), dy_t, hidden[:, :lent], outs[3:], 0)
        hidden_t[...] = hidden.T
        ggi_t[...] = ggi.T
        gl_t[...] = gl.T

    return kernel


def hidden_part(p, coords, hid, hid_t, dy, dy_t, gate_w, up_w, down_w):
    rows, width = hid.shape
    part = gate_w.shape[1] // RING
    lent = LENT if p == RING - 1 else 0

    def fixed(*shape):
        return pl.BlockSpec(shape, lambda i: (0, 0))

    weight = pl.BlockSpec((width, part), lambda i: (0, p))
    columns = 3 * part - lent
    shapes = [(part, rows)] * 3 + [(width // 4, columns)] * 2 + [(width // 2, columns)]
    shapes += [(width // 2, lent)] * 2 if lent else []
    return pl.pallas_call(
        hidden_kernel(p, lent),
        grid=(1,),
        out_shape=tuple(jax.ShapeDtypeStruct(shape, bf16) for shape in shapes),
        in_specs=[
            smem_spec(),
            fixed(rows, width),
            fixed(width, rows),
            fixed(rows, width),
            fixed(width, rows),
            weight,
            weight,
            weight,
        ],
        out_specs=tuple(fixed(*shape) for shape in shapes),
        compiler_params=limits(20),
        name="hidden_part",
    )(coords, hid, hid_t, dy, dy_t, gate_w, up_w, down_w)


def back_kernel(coords, *refs):
    acts, weights = refs[: 3 * RING], refs[3 * RING : 3 * RING + 3]
    outs, whole = refs[3 * RING + 3 : -1], refs[-1]
    feat, part = outs[0].shape[1], acts[0].shape[0]
    for j in range(3):
        for p in range(RING):
            whole[j, p * part : (p + 1) * part, :] = acts[j * RING + p][...]
    for other, out in ((1, outs[0]), (0, outs[1])):
        core = coords[3] if other == 0 else 1 - coords[3]

        def step(k, carry, core=core, out=out):
            block = 2 * ((coords[2] + k) & (RING - 1)) + core
            rows = pl.ds(pl.multiple_of(block * feat, feat), feat)
            terms = [
                jnp.dot(weight[rows, :], whole[j], preferred_element_type=f32)
                for j, weight in enumerate(weights)
            ]
            out[k] = (terms[0] + terms[1]).astype(bf16)
            out[RING + k] = terms[2].astype(bf16)
            return carry

        lax.fori_loop(0, RING, step, 0)


def back(coords, acts, weights):
    rows = acts[0][0].shape[1]
    feat = weights[0].shape[0] // (2 * RING)
    out = jax.ShapeDtypeStruct((2 * RING, feat, rows), bf16)
    return pl.pallas_call(
        back_kernel,
        in_specs=[smem_spec()] + [vmem_spec()] * (3 * RING + 3),
        out_specs=(vmem_spec(), vmem_spec()),
        out_shape=(out, out),
        scratch_shapes=[pltpu.VMEM((3, weights[0].shape[1], rows), bf16)],
        compiler_params=limits(20),
        name="back",
    )(coords, *[a for group in acts for a in group], *weights)


def chip_sum_kernel(near, other, own, *sends):
    feat = near.shape[1]
    for j in range(2):
        rows = slice(j * feat, (j + 1) * feat)
        own[rows, :] = near[j * RING].astype(f32) + other[j * RING].astype(f32)
        for k, send in enumerate(sends, 1):
            i = j * RING + k
            send[rows, :] = (near[i].astype(f32) + other[i].astype(f32)).astype(bf16)


def mp_scattered(far, near):
    other = lax.ppermute(far, "c", CORES)
    piece = (2 * near.shape[1], near.shape[2])
    own, *sends = pl.pallas_call(
        chip_sum_kernel,
        out_shape=(jax.ShapeDtypeStruct(piece, f32),)
        + (jax.ShapeDtypeStruct(piece, bf16),) * (RING - 1),
        in_specs=[vmem_spec()] * 2,
        out_specs=(vmem_spec(),) * RING,
        compiler_params=limits(8),
        name="chip_sum",
    )(near, other)
    came = []
    for k in (1, 3, 2):
        came.append(lax.ppermute(sends[k - 1], "y", shift(k)))
    return own, came


def split_kernel(*refs):
    ins, (send, kept) = refs[:-2], refs[-2:]
    half = send.shape[0]
    first = 0
    for keep, came in zip(ins[::2], ins[1::2]):
        columns = slice(first, first + keep.shape[1])
        send[:, columns] = (keep[:half, :].astype(f32) + came[:half, :].astype(f32)).astype(bf16)
        kept[:, columns] = (keep[half:, :].astype(f32) + came[half:, :].astype(f32)).astype(bf16)
        first += keep.shape[1]


def split_add(*pairs):
    rows = pairs[0].shape[0] // 2
    half = jax.ShapeDtypeStruct((rows, sum(a.shape[1] for a in pairs[::2])), bf16)
    return pl.pallas_call(
        split_kernel,
        out_shape=(half, half),
        in_specs=[vmem_spec()] * len(pairs),
        out_specs=(vmem_spec(),) * 2,
        compiler_params=limits(8),
        name="split_add",
    )(*pairs)


def half_kernel(half, count):
    def kernel(*refs):
        ins, outs = refs[:-count], refs[-count:]
        rows = ins[0].shape[0] // 2
        first = 0
        for keep, came in zip(ins[::2], ins[1::2]):
            mine = keep[half * rows : (half + 1) * rows, :]
            start = half * rows if came.shape[0] > rows else 0
            theirs = came[start : start + rows, :]
            columns = slice(first, first + keep.shape[1])
            total = (mine.astype(f32) + theirs.astype(f32)).astype(bf16)
            for i, out in enumerate(outs):
                out[:, columns] = total[i * out.shape[0] : (i + 1) * out.shape[0], :]
            first += keep.shape[1]

    return kernel


def half_add(half, count, *pairs):
    rows = pairs[0].shape[0] // 2 // count
    out = jax.ShapeDtypeStruct((rows, sum(a.shape[1] for a in pairs[::2])), bf16)
    return pl.pallas_call(
        half_kernel(half, count),
        out_shape=(out,) * count,
        in_specs=[vmem_spec()] * len(pairs),
        out_specs=(vmem_spec(),) * count,
        compiler_params=limits(6),
        name="half_add",
    )(*pairs)


def sections(part):
    runs = []
    for p in range(RING):
        lent = LENT if p == RING - 1 else 0
        runs.append([(0, p * part + lent, part - lent), (1, p * part, part), (2, p * part, part)])
    runs[0].append((0, (RING - 1) * part, LENT))
    return runs


def finish_kernel(*refs):
    inputs, ins = refs[:9], refs[9 : 9 + 2 * RING]
    out, grad_gain, *outs, acc = refs[9 + 2 * RING :]
    input_kernel(*inputs, out, grad_gain, acc)
    for p, runs in enumerate(sections(outs[0].shape[1] // RING)):
        total = ins[2 * p][...].astype(f32) + ins[2 * p + 1][...].astype(f32)
        first = 0
        for i, column, width in runs:
            outs[i][:, column : column + width] = total[:, first : first + width]
            first += width


def finished(groups, coords, tokens, cotangent, gain, table, grad, mine, came, pairs, width):
    rows, feat = tokens.shape
    out = jax.ShapeDtypeStruct((pairs[0][0].shape[0], width), f32)
    return pl.pallas_call(
        finish_kernel,
        out_shape=(
            jax.ShapeDtypeStruct((rows, feat), bf16),
            jax.ShapeDtypeStruct((1, feat), f32),
        )
        + (out,) * 3,
        in_specs=[smem_spec(), smem_spec()] + [vmem_spec()] * (7 + 2 * RING),
        out_specs=(vmem_spec(),) * 5,
        scratch_shapes=[pltpu.VMEM(table.shape, f32)],
        compiler_params=limits(12),
        name="finished",
    )(
        in_hbm(groups),
        coords,
        tokens,
        cotangent,
        gain,
        table,
        grad,
        mine,
        came,
        *[a for pair in pairs for a in pair],
    )


def body(tokens, norm_gain, running_sq, gate_weight, up_weight, down_weight_t, groups, cotangent):
    tok_rows, feat = tokens.shape
    groups_total = tok_rows * RING * RING // GHOST
    coords = jnp.stack([lax.axis_index(a) for a in ("z", "x", "y", "c")]).astype(jnp.int32)
    gain = norm_gain.reshape(1, -1)
    local, both = stats(groups, coords, tokens, cotangent, groups_total)
    pieces = gathered(both)
    sums = ring_pieces(ring_sum(local, "z"), "x")
    table, quad = scale_table(sums)
    tables = gathered(table)
    (down_weight_t,) = staged(down_weight_t)
    gate_weight, up_weight = staged(gate_weight, up_weight)
    dy_full, dy_turned = cotangent_whole(coords, pieces)
    hid_full, hid_turned = normalized_whole(groups, coords, gain, pieces, tables)
    parts = []
    for p in range(RING):
        parts.append(
            hidden_part(
                p, coords, hid_full, hid_turned, dy_full, dy_turned, gate_weight, up_weight, down_weight_t
            )
        )
    last = []
    for p, (major, first) in enumerate(PATTERNS):
        minor = "x" if major == "z" else "z"
        pair = (NEAR, FAR) if first == 0 else (FAR, NEAR)
        send_a, send_b, keep = parts[p][3:6]
        more = ()
        if p == 0:
            more = (parts[-1][7], lax.ppermute(parts[-1][6], major, pair[0]))
        came_a = lax.ppermute(send_a, major, pair[0])
        came_b = lax.ppermute(send_b, major, pair[0])
        send_a, send_b = half_add(0, 2, keep, came_a, *more)
        next_a = lax.ppermute(send_a, major, pair[1])
        next_b = lax.ppermute(send_b, major, pair[1])
        (keep,) = half_add(1, 1, keep, came_b, *more)
        (send,) = half_add(0, 1, keep, next_a)
        came = lax.ppermute(send, minor, pair[0])
        (keep,) = half_add(1, 1, keep, next_b)
        send, keep = split_add(keep, came)
        came = lax.ppermute(send, minor, pair[1])
        last.append((keep, came))
    far, near = back(
        coords,
        [[q[1] for q in parts], [q[2] for q in parts], [q[0] for q in parts]],
        [gate_weight, up_weight, down_weight_t],
    )
    kept, came_y = mp_scattered(far, near)
    grad, local = partials(groups, tokens, table, kept, came_y)
    mine, came = tok_halves(local)
    block_out, running_new = branch_out(tokens, running_sq.reshape(1, feat), quad, kept, came_y)
    grad_tokens, grad_gain, grad_down_t, grad_gate, grad_up = finished(
        groups, coords, tokens, cotangent, gain, table, grad, mine, came, last, gate_weight.shape[1]
    )
    return (
        block_out,
        grad_tokens,
        running_new.reshape(feat),
        grad_gain.reshape(feat),
        grad_gate,
        grad_up,
        grad_down_t,
    )


def solution(mesh):
    torus = Mesh(mesh.devices.reshape(RING, RING, RING, 2), ("z", "x", "y", "c"))
    tok, mp = ("z", "x"), ("y", "c")
    placed = (P(tok, mp), P(), P(mp), P(None, mp), P(None, mp), P(None, mp), P(tok), P(tok, mp))
    out = (P(tok, mp), P(tok, mp), P(mp), P(mp), P(tok, mp), P(tok, mp), P(tok, mp))

    return jax.shard_map(body, mesh=torus, in_specs=placed, out_specs=out, check_vma=False)
```
